256 devices in a mesh: seq: 64 (over y_hi, z, x), rep: 4 (over y_lo, core).
Axes of the slice: x: 4, y: 4 (y_hi: 2, y_lo: 2; y = y_hi * 2 + y_lo), z: 8, core: 2. Of those that a mesh axis runs over, the one named last changes fastest.
Arguments:
- queries: bfloat16 [32768, 4096], P(('rep', 'seq')), parts along dimension 0, may hold values from -160 to 160
- keys_values: bfloat16 [2, 32768, 1024], P(None, ('rep', 'seq')), parts along dimension 1, may hold values from -6 to 6
- segment_ids: int32 [32768], P(('rep', 'seq')), parts along dimension 0, may hold values from 0 to 31, never falling along the last dimension, each value on 1 to 4096 neighbouring positions
Outputs:
- attended: bfloat16 [32768, 4096], P(('rep', 'seq')), parts along dimension 0
The draws below stay inside these ranges and needn't reach their ends.
There are 4 independent parts, one for each index of `rep`. The reference program is written for one: setup_inputs(seed, part) draws one part's arguments, and reference() takes and returns one part's arrays. A program takes and returns all parts, laid end to end along the dimension named above; each array names one. Nothing has to cross between parts.
Inputs may be any that keep to these rules, and one draw needn't show every extreme that they name: `segment_ids`: ids never fall along the tokens; every document holds 1 to 4096 consecutive tokens, one exactly 4096.
All inputs are finite; a program needn't handle non-finite values.
Results may differ from the reference program's by a relative error of at most 0.004.
Values may be sent and summed in bfloat16 or wider, within the bound.
A program may use at most 192 MiB of HBM per device.

```python
import math
import jax
import jax.numpy as jnp
import numpy as np
from jax import lax

HQ = 32
HK = 8
DH = 128
WINDOW = 2048
DOC_COUNT = 32
TOKENS = 8192
DOC_MOST = 4096


def shared_draw(key):
    shape_keys = (TOKENS, HK * DH)
    key_rows = jnp.clip(jax.random.normal(jax.random.fold_in(key, 101), shape_keys, jnp.float32), -6.0, 6.0)
    value_rows = jnp.clip(jax.random.normal(jax.random.fold_in(key, 102), shape_keys, jnp.float32), -6.0, 6.0)
    query_rows = jnp.clip(jax.random.normal(jax.random.fold_in(key, 103), (TOKENS, HQ * DH), jnp.float32), -6.0, 6.0)
    return (query_rows, jnp.stack([key_rows, value_rows]))


def draw_queries(key, part):
    return shared_draw(key)[0].astype(jnp.bfloat16)


def draw_keys_values(key, part):
    return shared_draw(key)[1].astype(jnp.bfloat16)


def length_profile(amount, total, limit, slope):
    weights = [(1 << 20) // math.isqrt(standing ** slope) + 1 for standing in range(2, amount + 1)]
    spare, given = total - limit - (amount - 1), [1] * (amount - 1)
    while spare > 0:
        free = [i for i in range(amount - 1) if given[i] < limit]
        whole, budget = sum([weights[i] for i in free]), spare
        for i in free:
            addition = min(limit - given[i], max(1, budget * weights[i] // whole), spare)
            given[i] = given[i] + addition
            spare = spare - addition
    return np.array([limit] + given)


def uneven_parts(own_key, number_of, total, limit, skew):
    if number_of == 2:
        one = jax.random.randint(own_key, (), max(1, total - limit), min(limit, total - 1) + 1)
        return jnp.stack([one, total - one])
    tallies = jnp.asarray(length_profile(number_of, total, limit, skew), jnp.int32)
    couples = (number_of - 1) // 2
    donor, receiver = tallies[1:1 + 2 * couples:2], tallies[2:2 + 2 * couples:2]
    room = jnp.minimum(donor - 1, limit - receiver)
    moved = jax.random.randint(jax.random.fold_in(own_key, 1), (couples,), 0, 1 << 20) % (room + 1)
    tallies = tallies.at[1:1 + 2 * couples:2].set(donor - moved).at[2:2 + 2 * couples:2].set(receiver + moved)
    return tallies[jax.random.permutation(jax.random.fold_in(own_key, 2), number_of)]


def setup_inputs(seed: int = 0, part: int = 0) -> dict:
    streams_of = jax.random.split(jax.random.key(seed), 4)
    part_keys = jax.random.split(jax.random.fold_in(streams_of[3], part), 4)
    queries = draw_queries(jax.random.fold_in(jax.random.fold_in(streams_of[3], part), 71), part)
    keys_values = draw_keys_values(jax.random.fold_in(jax.random.fold_in(streams_of[3], part), 71), part)
    segment_ids = jnp.searchsorted(jnp.cumsum(uneven_parts(part_keys[2], DOC_COUNT, TOKENS, DOC_MOST, 2)), jnp.arange(TOKENS), side="right").astype(jnp.int32)
    return dict(queries=queries, keys_values=keys_values, segment_ids=segment_ids)


def reference(queries, keys_values, segment_ids):
    group_size = HQ // HK
    score_scale = DH ** -0.5
    query_rows = min(512, TOKENS)
    key_span = WINDOW + query_rows
    key_table = jnp.pad(keys_values[0], ((WINDOW, 0), (0, 0)))
    value_table = jnp.pad(keys_values[1], ((WINDOW, 0), (0, 0)))
    padded_ids = jnp.pad(segment_ids, (WINDOW, 0), constant_values=-1)

    def one_block(number):
        first_row = (number * query_rows).astype(jnp.int32)
        query_block = lax.dynamic_slice_in_dim(queries, first_row, query_rows, 0)
        query_block = query_block.reshape(query_rows, HK, group_size, DH).astype(jnp.float32)
        key_block = lax.dynamic_slice_in_dim(key_table, first_row, key_span, 0).reshape(key_span, HK, DH).astype(jnp.float32)
        value_block = lax.dynamic_slice_in_dim(value_table, first_row, key_span, 0).reshape(key_span, HK, DH).astype(jnp.float32)
        query_ids = lax.dynamic_slice_in_dim(segment_ids, first_row, query_rows, 0)
        key_ids = lax.dynamic_slice_in_dim(padded_ids, first_row, key_span, 0)
        query_place = jnp.arange(query_rows, dtype=jnp.int32) + WINDOW
        key_place = jnp.arange(key_span, dtype=jnp.int32)
        distance = query_place[:, None] - key_place[None, :]
        allowed = (query_ids[:, None] == key_ids[None, :]) & (distance >= 0) & (distance < WINDOW)
        scores = jnp.einsum("qhgd,khd->hgqk", query_block, key_block) * score_scale
        scores = jnp.where(allowed, scores, -1.0e30)
        top = jnp.max(scores, axis=-1, keepdims=True)
        weights = jnp.where(allowed, jnp.exp(scores - top), 0.0)
        totals = jnp.sum(weights, axis=-1)
        rounded = lax.optimization_barrier(weights.astype(jnp.bfloat16))
        context = jnp.einsum("hgqk,khd->hgqd", rounded.astype(jnp.float32), value_block)
        result = context / totals[..., None]
        return jnp.transpose(result, (2, 0, 1, 3)).reshape(query_rows, HQ * DH).astype(jnp.bfloat16)

    blocks = lax.map(one_block, jnp.arange(TOKENS // query_rows, dtype=jnp.int32))
    return blocks.reshape(TOKENS, HQ * DH)
```

```python
import math

import jax
import jax.numpy as jnp
from jax import lax
from jax.experimental import pallas as pl
from jax.experimental.pallas import tpu as pltpu
from jax.sharding import PartitionSpec as P

HQ = 32
HK = 8
DH = 128
WINDOW = 2048

RING = 4
ROWS = 128
PLANE = RING * ROWS
SLOTS = WINDOW // PLANE + 1
GROUP = HQ // HK
HEADS = HK // RING
WIDE = GROUP * DH
NEG_BIG = -1e30
SCALE = DH**-0.5 * math.log2(math.e)
MESH = pl.DeviceIdType.MESH


def kernel(
    q_hbm, kv_hbm, id_in, o_hbm,
    qbuf, kvb, idb, qidc, m_sc, l_sc, acc_sc, obuf,
    loc_sem, kvx_ss, kv_rs, z_ss, qx_ss, q_rs, idx_ss, id0_rs, idz_ss, idz_rs, o_ss, o_rs,
):
    planes = lax.axis_size("seq") // RING
    me = lax.axis_index("seq")
    x = lax.rem(me, RING)
    plane = me // RING
    has_next = plane < planes - 1
    has_prev = plane > 0
    ring_base = plane * RING
    nxt = lax.rem(me + RING, planes * RING)
    prv = lax.rem(me + (planes - 1) * RING, planes * RING)

    def partner(d):
        return lax.rem(x + d, RING)

    def remote(src, dst, ss, rs, seq):
        return pltpu.make_async_remote_copy(
            src_ref=src, dst_ref=dst, send_sem=ss, recv_sem=rs,
            device_id={"seq": seq}, device_id_type=MESH,
        )

    def kv_src(px, a):
        return kv_hbm.at[:, :, pl.ds(pl.multiple_of((px * HEADS + a) * DH, DH), DH)]

    def q_src(px, a):
        return q_hbm.at[:, pl.ds(pl.multiple_of((px * HEADS + a) * WIDE, WIDE), WIDE)]

    def chunk(a, slot, c):
        return kvb.at[a, slot, :, pl.ds(pl.multiple_of(c * ROWS, ROWS), ROWS), :]

    local = []
    for a in range(HEADS):
        local.append(pltpu.make_async_copy(kv_src(x, a), chunk(a, 0, x), loc_sem.at[a]))
        local.append(pltpu.make_async_copy(q_src(x, a), qbuf.at[a, x], loc_sem.at[HEADS + a]))
    for cp in local:
        cp.start()
    idb[0, x] = id_in[...]

    barrier = pltpu.get_barrier_semaphore()
    for d in range(1, RING):
        pl.semaphore_signal(barrier, inc=1, device_id={"seq": ring_base + partner(d)}, device_id_type=MESH)

    @pl.when(has_prev)
    def _():
        pl.semaphore_signal(barrier, inc=1, device_id={"seq": prv}, device_id_type=MESH)

    @pl.when(has_next)
    def _():
        pl.semaphore_wait(barrier, RING)

    @pl.when(jnp.logical_not(has_next))
    def _():
        pl.semaphore_wait(barrier, RING - 1)

    def id_send(d):
        return remote(id_in, idb.at[0, x], idx_ss.at[d - 1], id0_rs.at[x], ring_base + partner(d))

    def kv_send(a, d):
        px = partner(d)
        return remote(kv_src(px, a), chunk(a, 0, x), kvx_ss.at[a, d - 1], kv_rs.at[a, 0, x], ring_base + px)

    def q_send(a, d):
        px = partner(d)
        return remote(q_src(px, a), qbuf.at[a, x], qx_ss.at[a, d - 1], q_rs.at[a, x], ring_base + px)

    def own_forward(a):
        return remote(kv_src(x, a), chunk(a, 1, x), z_ss.at[a, 0, x], kv_rs.at[a, 1, x], nxt)

    def forward(a, slot, c):
        return remote(chunk(a, slot, c), chunk(a, slot + 1, c), z_ss.at[a, slot, c], kv_rs.at[a, slot + 1, c], nxt)

    def id_forward(slot):
        return remote(idb.at[slot], idb.at[slot + 1], idz_ss.at[slot], idz_rs.at[slot + 1], nxt)

    def arrived(a, slot, c):
        return remote(chunk(a, slot, c), chunk(a, slot, c), kvx_ss.at[0, 0], kv_rs.at[a, slot, c], nxt)

    @pl.when(has_next)
    def _():
        own_forward(0).start()

    for d in range(1, RING):
        id_send(d).start()
    for d in range(1, RING):
        kv_send(0, d).start()
    for d in range(1, RING):
        q_send(0, d).start()
    for a in range(1, HEADS):
        for d in range(1, RING):
            kv_send(a, d).start()
        for d in range(1, RING):
            q_send(a, d).start()

    def receive(e):
        step, j = e // RING, lax.rem(e, RING)
        a, slot = step // SLOTS, lax.rem(step, SLOTS)
        c = lax.rem(x + j, RING)

        @pl.when(jnp.logical_and(a == 0, j == 0))
        def _():
            @pl.when(slot == 0)
            def _():
                for d in range(1, RING):
                    pc = partner(d)
                    remote(idb.at[0, pc], idb.at[0, pc], idx_ss.at[0], id0_rs.at[pc], nxt).wait_recv()

            @pl.when(jnp.logical_and(slot > 0, slot <= plane))
            def _():
                remote(idb.at[slot], idb.at[slot], idx_ss.at[0], idz_rs.at[slot], nxt).wait_recv()

            @pl.when(jnp.logical_and(has_next, jnp.logical_and(slot <= plane, slot < SLOTS - 1)))
            def _():
                id_forward(slot).start()

        @pl.when(jnp.logical_and(slot == 0, j == 0))
        def _():
            pltpu.make_async_copy(kv_src(x, a), chunk(a, 0, x), loc_sem.at[a]).wait()

            @pl.when(jnp.logical_and(has_next, a > 0))
            def _():
                own_forward(a).start()

        @pl.when(jnp.logical_and(slot <= plane, jnp.logical_or(slot > 0, j > 0)))
        def _():
            arrived(a, slot, c).wait_recv()

            @pl.when(jnp.logical_and(has_next, slot < SLOTS - 1))
            def _():
                forward(a, slot, c).start()

    row = lax.broadcasted_iota(jnp.int32, (ROWS, ROWS), 0)
    col = lax.broadcasted_iota(jnp.int32, (ROWS, ROWS), 1)

    def piece(n):
        step, j = n // RING, lax.rem(n, RING)
        a, slot = step // SLOTS, lax.rem(step, SLOTS)
        qb = lax.rem(x + 1 + j, RING)

        @pl.when(slot == 0)
        def _():
            @pl.when(j < RING - 1)
            def _():
                remote(qbuf.at[a, qb], qbuf.at[a, qb], idx_ss.at[0], q_rs.at[a, qb], nxt).wait_recv()

            @pl.when(j == RING - 1)
            def _():
                pltpu.make_async_copy(q_src(x, a), qbuf.at[a, x], loc_sem.at[HEADS + a]).wait()

            m_sc[qb] = jnp.full((GROUP * ROWS, DH), NEG_BIG, jnp.float32)
            l_sc[qb] = jnp.zeros((GROUP * ROWS, DH), jnp.float32)
            acc_sc[qb] = jnp.zeros((GROUP * ROWS, DH), jnp.float32)
            qidc[qb] = jnp.transpose(jnp.broadcast_to(idb[0, qb], (ROWS, ROWS)))

        @pl.when(slot <= plane)
        def _():
            query_ids = qidc[qb]
            bias = []
            for c in range(RING):
                distance = row - col + (slot * PLANE + (qb - c) * ROWS)
                keep = (query_ids == idb[slot, c]) & (distance >= 0) & (distance < WINDOW)
                bias.append(jnp.where(keep, 0.0, NEG_BIG))
            bias = jnp.concatenate(bias, axis=1)
            q_all = qbuf[a, qb]
            q4 = jnp.concatenate([q_all[:, g * DH : (g + 1) * DH] for g in range(GROUP)], axis=0)
            keys = kvb[a, slot, 0]
            values = kvb[a, slot, 1]
            s = lax.dot_general(q4, keys, (((1,), (1,)), ((), ())), preferred_element_type=jnp.float32)
            s = s + jnp.concatenate([bias] * GROUP, axis=0)
            m_prev = m_sc[qb]
            m_new = jnp.maximum(m_prev, jnp.max(s, axis=1, keepdims=True))
            alpha = jnp.exp2((m_prev - m_new) * SCALE)
            p = jnp.exp2((s - jnp.concatenate([m_new] * RING, axis=1)) * SCALE)
            part = p[:, :ROWS]
            for c in range(1, RING):
                part = part + p[:, c * ROWS : (c + 1) * ROWS]
            l_sc[qb] = l_sc[qb] * alpha + part
            acc_sc[qb] = acc_sc[qb] * alpha + jnp.dot(
                p.astype(jnp.bfloat16), values, preferred_element_type=jnp.float32
            )
            m_sc[qb] = m_new

        @pl.when(slot == SLOTS - 1)
        def _():
            out = acc_sc[qb] / jnp.sum(l_sc[qb], axis=1, keepdims=True)
            for g in range(GROUP):
                obuf[a, qb, :, g * DH : (g + 1) * DH] = out[g * ROWS : (g + 1) * ROWS].astype(jnp.bfloat16)

            @pl.when(j < RING - 1)
            def _():
                o_send(a, qb).start()

            @pl.when(j == RING - 1)
            def _():
                o_local(a).start()

    def o_dst(px, a):
        return o_hbm.at[:, pl.ds(pl.multiple_of((px * HEADS + a) * WIDE, WIDE), WIDE)]

    def o_send(a, qb):
        return remote(obuf.at[a, qb], o_dst(x, a), o_ss.at[a, qb], o_rs.at[a, x], ring_base + qb)

    def o_local(a):
        return pltpu.make_async_copy(obuf.at[a, x], o_dst(x, a), loc_sem.at[2 * HEADS + a])

    events = HEADS * SLOTS * RING

    def done(e):
        return jnp.maximum(0, jnp.minimum(2 * (e - 7), e - 3))

    def event(e, carry):
        receive(e)

        def inner(n, c):
            piece(n)
            return c

        lax.fori_loop(done(e - 1), done(e), inner, 0)
        return carry

    lax.fori_loop(0, events, event, 0)

    def tail(n, c):
        piece(n)
        return c

    lax.fori_loop(events - RING, events, tail, 0)

    for a in range(HEADS):
        for d in range(1, RING):
            kv_send(a, d).wait_send()
            q_send(a, d).wait_send()
            pc = partner(d)
            o_send(a, pc).wait_send()
            remote(o_dst(pc, a), o_dst(pc, a), idx_ss.at[0], o_rs.at[a, pc], nxt).wait_recv()
        o_local(a).wait()
    for d in range(1, RING):
        id_send(d).wait_send()

    @pl.when(has_next)
    def _():
        def drain(n, c):
            a, k = n // (RING * (SLOTS - 1)), lax.rem(n, RING * (SLOTS - 1))
            slot, cc = k // RING, lax.rem(k, RING)

            @pl.when(slot <= plane)
            def _():
                forward(a, slot, cc).wait_send()

            return c

        lax.fori_loop(0, HEADS * RING * (SLOTS - 1), drain, 0)
        for slot in range(SLOTS - 1):
            @pl.when(slot <= plane)
            def _():
                id_forward(slot).wait_send()


def local(queries, keys_values, segment_ids):
    dma = pltpu.SemaphoreType.DMA
    return pl.pallas_call(
        kernel,
        out_shape=jax.ShapeDtypeStruct(queries.shape, queries.dtype),
        in_specs=[
            pl.BlockSpec(memory_space=pl.ANY),
            pl.BlockSpec(memory_space=pl.ANY),
            pl.BlockSpec(memory_space=pltpu.VMEM),
        ],
        out_specs=pl.BlockSpec(memory_space=pl.ANY),
        scratch_shapes=[
            pltpu.VMEM((HEADS, RING, ROWS, WIDE), jnp.bfloat16),
            pltpu.VMEM((HEADS, SLOTS, 2, PLANE, DH), jnp.bfloat16),
            pltpu.VMEM((SLOTS, RING, 1, ROWS), jnp.int32),
            pltpu.VMEM((RING, ROWS, ROWS), jnp.int32),
            pltpu.VMEM((RING, GROUP * ROWS, DH), jnp.float32),
            pltpu.VMEM((RING, GROUP * ROWS, DH), jnp.float32),
            pltpu.VMEM((RING, GROUP * ROWS, DH), jnp.float32),
            pltpu.VMEM((HEADS, RING, ROWS, WIDE), jnp.bfloat16),
            dma((3 * HEADS,)),
            dma((HEADS, RING - 1)),
            dma((HEADS, SLOTS, RING)),
            dma((HEADS, SLOTS - 1, RING)),
            dma((HEADS, RING - 1)),
            dma((HEADS, RING)),
            dma((RING - 1,)),
            dma((RING,)),
            dma((SLOTS - 1,)),
            dma((SLOTS,)),
            dma((HEADS, RING)),
            dma((HEADS, RING)),
        ],
        compiler_params=pltpu.CompilerParams(collective_id=0, has_side_effects=True),
        name="window_attention",
    )(queries, keys_values, segment_ids.reshape(1, ROWS))


def solution(mesh):
    return jax.shard_map(
        local,
        mesh=mesh,
        in_specs=(P(("rep", "seq"), None), P(None, ("rep", "seq"), None), P(("rep", "seq"))),
        out_specs=P(("rep", "seq"), None),
        check_vma=False,
    )
```

```python
import math

import jax
import jax.numpy as jnp
from jax import lax
from jax.experimental import pallas as pl
from jax.experimental.pallas import tpu as pltpu
from jax.sharding import PartitionSpec as P

HQ = 32
HK = 8
DH = 128
WINDOW = 2048

RING = 4
ROWS = 128
PLANE = RING * ROWS
SLOTS = WINDOW // PLANE + 1
GROUP = HQ // HK
HEADS = HK // RING
WIDE = GROUP * DH
NEG_BIG = -1e30
SCALE = DH**-0.5 * math.log2(math.e)
MESH = pl.DeviceIdType.MESH
ZRING = 8
PLANES = 16
BACK = HEADS - 1
BACKS = RING - 1
LAST_BACK = PLANES - 3
F_EVENTS = 24
R_LAG = 4
R_EARLY = 4
R_LATE = 4


def kernel(
    q_hbm, kv_hbm, id_in, o_hbm,
    qbuf, kvb, rel, idb, qidc, m_sc, l_sc, acc_sc, obuf,
    loc_sem, kvx_ss, kv_rs, z_ss, qx_ss, q_rs, idx_ss, id0_rs, idz_ss, idz_rs, o_ss, o_rs,
    back_ss, rel_ss, rel_rs, rz_ss, ext, ext_ss, ext_rs,
):
    me = lax.axis_index("seq")
    x = lax.rem(me, RING)
    plane = me // RING
    half = plane // ZRING
    z = lax.rem(plane, ZRING)
    has_next = plane < PLANES - 1
    ring_base = plane * RING
    nxt = lax.rem(me + RING, PLANES * RING)
    prv = lax.rem(me + (PLANES - 1) * RING, PLANES * RING)

    def around(k):
        return half * ZRING + lax.rem(z + k, ZRING)

    down = around(ZRING - 1) * RING + x
    up = around(1) * RING + x

    def partner(d):
        return lax.rem(x + d, RING)

    def remote(src, dst, ss, rs, seq):
        return pltpu.make_async_remote_copy(
            src_ref=src, dst_ref=dst, send_sem=ss, recv_sem=rs,
            device_id={"seq": seq}, device_id_type=MESH,
        )

    def kv_src(px, a):
        return kv_hbm.at[:, :, pl.ds(pl.multiple_of((px * HEADS + a) * DH, DH), DH)]

    def q_src(px, a):
        return q_hbm.at[:, pl.ds(pl.multiple_of((px * HEADS + a) * WIDE, WIDE), WIDE)]

    def o_dst(px, a):
        return o_hbm.at[:, pl.ds(pl.multiple_of((px * HEADS + a) * WIDE, WIDE), WIDE)]

    def rows(c):
        return pl.ds(c * ROWS if isinstance(c, int) else pl.multiple_of(c * ROWS, ROWS), ROWS)

    def chunk(a, slot, c):
        return kvb.at[a, slot, :, rows(c), :]

    def signal(sem, seq):
        pl.semaphore_signal(sem, inc=1, device_id={"seq": seq}, device_id_type=MESH)

    def when(cond):
        return pl.when(cond)

    kv_local = [pltpu.make_async_copy(kv_src(x, a), chunk(a, 0, x), loc_sem.at[a]) for a in range(HEADS)]
    q_local = [pltpu.make_async_copy(q_src(x, a), qbuf.at[a, x], loc_sem.at[HEADS + a]) for a in range(HEADS)]
    for cp in kv_local + q_local:
        cp.start()
    idb[0, x] = id_in[...]

    barrier = pltpu.get_barrier_semaphore()
    third = around(3)
    for d in range(1, RING):
        signal(barrier, ring_base + partner(d))
    signal(barrier, up)

    @when(plane > 0)
    def _():
        signal(barrier, prv)

    def last_relay(source):
        h = source // ZRING
        return (h * ZRING + lax.rem(source + ZRING - 3, ZRING)) * RING + x

    @when(plane >= SLOTS - 1)
    def _():
        signal(barrier, last_relay(plane - (SLOTS - 1)))

    @when(plane == PLANES - 1)
    def _():
        signal(barrier, last_relay(PLANES - 4))
        signal(barrier, last_relay(PLANES - 3))

    @when(jnp.logical_and(jnp.logical_and(plane >= 2, plane != ZRING - 1), has_next))
    def _():
        signal(barrier, nxt)

    targets = (has_next, third <= LAST_BACK, jnp.logical_and(plane >= 3, plane != ZRING))
    count = jnp.int32(RING)
    for target in targets:
        count = count + jnp.where(target, 1, 0)
    pl.semaphore_wait(barrier, count)

    def id_send(d):
        return remote(id_in, idb.at[0, x], idx_ss.at[d - 1], id0_rs.at[x], ring_base + partner(d))

    def kv_send(a, d):
        px = partner(d)
        return remote(kv_src(px, a), chunk(a, 0, x), kvx_ss.at[a, d - 1], kv_rs.at[a, 0, x], ring_base + px)

    def q_send(a, d):
        px = partner(d)
        return remote(q_src(px, a), qbuf.at[a, x], qx_ss.at[a, d - 1], q_rs.at[a, x], ring_base + px)

    def own_forward(a):
        return remote(kv_src(x, a), chunk(a, 1, x), z_ss.at[a, 0, x], kv_rs.at[a, 1, x], nxt)

    def forward(a, slot, c):
        return remote(chunk(a, slot, c), chunk(a, slot + 1, c), z_ss.at[a, slot, c], kv_rs.at[a, slot + 1, c], nxt)

    def id_forward(slot):
        return remote(idb.at[slot], idb.at[slot + 1], idz_ss.at[slot], idz_rs.at[slot + 1], nxt)

    def wait_chunk(a, slot, c):
        remote(chunk(a, slot, c), chunk(a, slot, c), kvx_ss.at[0, 0], kv_rs.at[a, slot, c], nxt).wait_recv()

    def back_own(k):
        return remote(chunk(BACK, 0, k + 1), rel.at[0, k], back_ss.at[k], rel_rs.at[0, k], down)

    def back_relay(i, k):
        if i < 2:
            return remote(rel.at[i, k], rel.at[i + 1, k], rel_ss.at[i, k], rel_rs.at[i + 1, k], down)
        over = jnp.maximum(third - (PLANES - SLOTS), 0)
        slot = SLOTS - 1 - over
        first = jnp.minimum(third + SLOTS - 1, PLANES - 1) * RING + x
        return remote(rel.at[i, k], chunk(BACK, slot, k + 1), rel_ss.at[i, k], kv_rs.at[BACK, slot, k + 1], first)

    def back_next(slot, k):
        return remote(
            chunk(BACK, slot, k + 1), chunk(BACK, slot - 1, k + 1),
            rz_ss.at[slot - 3, k], kv_rs.at[BACK, slot - 1, k + 1], prv,
        )

    def ext_down(e, k, src):
        return remote(src, ext.at[e, k], ext_ss.at[e, k], ext_rs.at[e, k], down)

    def ext_last(e, k):
        slot = 3 - e
        return remote(ext.at[e, k], chunk(BACK, slot, k + 1), ext_ss.at[e, k], kv_rs.at[BACK, slot, k + 1], down)

    def wait_ext(e, k):
        remote(ext.at[e, k], ext.at[e, k], idx_ss.at[0], ext_rs.at[e, k], nxt).wait_recv()

    def o_send(a, qb):
        return remote(obuf.at[a, qb], o_dst(x, a), o_ss.at[a, qb], o_rs.at[a, x], ring_base + qb)

    def o_local(a):
        return pltpu.make_async_copy(obuf.at[a, x], o_dst(x, a), loc_sem.at[2 * HEADS + a])

    @when(has_next)
    def _():
        for a in range(HEADS):
            own_forward(a).start()

    for d in range(1, RING):
        id_send(d).start()
    for a in range(HEADS):
        for d in (1, 3, 2):
            kv_send(a, d).start()
    for a in range(HEADS):
        for d in (1, 3, 2):
            q_send(a, d).start()

    kv_local[0].wait()
    for j in (1, 3, 2):
        wait_chunk(0, 0, partner(j))

        @when(has_next)
        def _():
            forward(0, 0, partner(j)).start()

    for d in range(1, RING):
        pc = partner(d)
        remote(idb.at[0, pc], idb.at[0, pc], idx_ss.at[0], id0_rs.at[pc], nxt).wait_recv()

    @when(has_next)
    def _():
        id_forward(0).start()

    kv_local[1].wait()
    for j in (1, 3, 2):
        wait_chunk(1, 0, partner(j))

    @when(plane <= LAST_BACK)
    def _():
        for k in range(BACKS):
            back_own(k).start()

    @when(jnp.logical_and(has_next, x != 0))
    def _():
        forward(1, 0, 0).start()

    def f_event(n):
        if n < 5:
            a, slot, c = (0, 1, x) if n == 0 else (1, 1, x) if n == 1 else (0, 1, partner((1, 3, 2)[n - 2]))
        elif n < 21:
            k = n - 6
            a, slot, c = 0, 2 + k // 5, partner((0, 1, 3, 2, 0)[k % 5])
            if n % 5 == 0:
                a, slot, c = 1, n // 5, 0
        else:
            a, slot, c = 1, 1, n - 20
        if n in (0, 6, 11, 16):
            @when(plane >= slot)
            def _():
                remote(idb.at[slot], idb.at[slot], idx_ss.at[0], idz_rs.at[slot], nxt).wait_recv()

                if slot < SLOTS - 1:
                    @when(has_next)
                    def _():
                        id_forward(slot).start()

        there = plane >= slot
        if n == 5 or n > 20:
            there = jnp.logical_and(there, c != x)

        @when(there)
        def _():
            wait_chunk(a, slot, c)

        if slot < SLOTS - 1 and n != 1 and n <= 20:
            @when(jnp.logical_and(plane >= slot, has_next))
            def _():
                forward(a, slot, c).start()

        if n == 15:
            for cc in range(1, RING):
                @when(jnp.logical_and(has_next, cc != x))
                def _():
                    forward(1, 0, cc).start()

    def r_event(m):
        d, k = 1 + m // BACKS, m % BACKS
        if d <= 3:
            @when(around(d) <= LAST_BACK)
            def _():
                remote(rel.at[d - 1, k], rel.at[d - 1, k], idx_ss.at[0], rel_rs.at[d - 1, k], nxt).wait_recv()
                back_relay(d - 1, k).start()

            if d == 3:
                for e in range(2):
                    @when(plane == 1 + e)
                    def _():
                        ext_down(e, k, rel.at[2, k]).start()
        else:
            slot = 8 - d

            @when(plane >= slot)
            def _():
                wait_chunk(BACK, slot, k + 1)

                if slot > 2:
                    @when(plane != ZRING)
                    def _():
                        back_next(slot, k).start()

            if d == 4:
                @when(plane == 1)
                def _():
                    wait_ext(1, k)
                    ext_down(1, k, ext.at[1, k]).start()

            if d < 6:
                @when(plane == 0)
                def _():
                    wait_ext(d - 4, k)
                    ext_last(d - 4, k).start()

    row = lax.broadcasted_iota(jnp.int32, (ROWS, ROWS), 0)
    col = lax.broadcasted_iota(jnp.int32, (ROWS, ROWS), 1)

    def start_block(a, qb):
        @when(qb != x)
        def _():
            remote(qbuf.at[a, qb], qbuf.at[a, qb], idx_ss.at[0], q_rs.at[a, qb], nxt).wait_recv()

        @when(qb == x)
        def _():
            q_local[a].wait()

        m_sc[a, qb] = jnp.full((GROUP * ROWS, DH), NEG_BIG, jnp.float32)
        l_sc[a, qb] = jnp.zeros((GROUP * ROWS, DH), jnp.float32)
        acc_sc[a, qb] = jnp.zeros((GROUP * ROWS, DH), jnp.float32)
        if a == 0:
            qidc[qb] = jnp.transpose(jnp.broadcast_to(idb[0, qb], (ROWS, ROWS)))

    def block(a, slot, qb, c0, c1):
        query_ids = qidc[qb]
        bias = []
        for c in range(c0, c1):
            keep = query_ids == idb[slot, c]
            if slot == 0 and isinstance(qb, int) and c == qb:
                keep = keep & (row >= col)
            if slot == SLOTS - 1 and isinstance(qb, int) and c == qb:
                keep = keep & (col > row)
            bias.append(jnp.where(keep, 0.0, NEG_BIG))
        bias = jnp.concatenate(bias, axis=1)
        q_all = qbuf[a, qb]
        q4 = jnp.concatenate([q_all[:, g * DH : (g + 1) * DH] for g in range(GROUP)], axis=0)
        span = slice(c0 * ROWS, c1 * ROWS)
        keys = kvb[a, slot, 0, span, :]
        values = kvb[a, slot, 1, span, :]
        s = lax.dot_general(q4, keys, (((1,), (1,)), ((), ())), preferred_element_type=jnp.float32)
        s = s + jnp.concatenate([bias] * GROUP, axis=0)
        m_prev = m_sc[a, qb]
        m_new = jnp.maximum(m_prev, jnp.max(s, axis=1, keepdims=True))
        alpha = jnp.exp2((m_prev - m_new) * SCALE)
        p = jnp.exp2((s - jnp.concatenate([m_new] * (c1 - c0), axis=1)) * SCALE)
        part = p[:, :ROWS]
        for c in range(1, c1 - c0):
            part = part + p[:, c * ROWS : (c + 1) * ROWS]
        l_sc[a, qb] = l_sc[a, qb] * alpha + part
        acc_sc[a, qb] = acc_sc[a, qb] * alpha + jnp.dot(
            p.astype(jnp.bfloat16), values, preferred_element_type=jnp.float32
        )
        m_sc[a, qb] = m_new

    def inner(a, slot, lo, hi, c0=0):
        @when(plane >= slot)
        def _():
            def one(qb, carry):
                block(a, slot, qb, c0, RING)
                return carry

            lax.fori_loop(lo, hi, one, 0)

    def diagonal(a, lo, hi):
        for qb in range(lo, hi):
            start_block(a, qb)
            block(a, 0, qb, 0, qb + 1)

    def edge(a, lo, hi, c0=0):
        @when(plane >= SLOTS - 1)
        def _():
            for qb in range(lo, hi):
                block(a, SLOTS - 1, qb, max(qb, c0), RING)

    def first_chunk(slot, lo, hi):
        @when(plane >= slot)
        def _():
            for qb in range(lo, hi):
                block(BACK, slot, qb, 0, 1)

    def finish(a, lo, hi):
        for qb in range(lo, hi):
            out = acc_sc[a, qb] / jnp.sum(l_sc[a, qb], axis=1, keepdims=True)
            for g in range(GROUP):
                obuf[a, qb, :, g * DH : (g + 1) * DH] = out[g * ROWS : (g + 1) * ROWS].astype(jnp.bfloat16)

            @when(qb != x)
            def _():
                o_send(a, qb).start()

            @when(qb == x)
            def _():
                o_local(a).start()

    def near(lo, hi):
        @when(plane >= 1)
        def _():
            def one(qb, carry):
                block(BACK, 1, qb, lo, hi)
                return carry

            lax.fori_loop(0, RING, one, 0)

    work = {
        6: [lambda: diagonal(0, 0, 4)],
        7: [lambda: inner(0, 1, 0, 2)],
        8: [lambda: inner(0, 1, 2, 4)],
        10: [lambda: inner(0, 2, 0, 2)],
        11: [lambda: inner(0, 2, 2, 4)],
        12: [lambda: diagonal(1, 0, 2)],
        13: [lambda: diagonal(1, 2, 4)],
        15: [lambda: inner(0, 3, 0, 2)],
        16: [lambda: inner(0, 3, 2, 4)],
        18: [lambda: inner(1, 3, 0, 4)],
        19: [lambda: edge(0, 0, 4), lambda: finish(0, 0, 4)],
        20: [lambda: edge(1, 0, 4)],
        21: [lambda: inner(1, 2, 0, 4)],
        22: [lambda: near(0, 3)],
        23: [lambda: near(3, 4), lambda: finish(1, 0, 4)],
    }
    early = plane == ZRING
    late = jnp.logical_or(plane == ZRING - 1, plane == ZRING - 2)
    lags = (
        (R_EARLY, early),
        (R_LATE, late),
        (R_LAG, jnp.logical_not(jnp.logical_or(early, late))),
    )
    for n in range(F_EVENTS):
        for lag, mine in lags:
            ms = range(0, n - lag + 1) if n == 0 else (n - lag,)
            for m in ms:
                if 0 <= m < 6 * BACKS:
                    @when(mine)
                    def _():
                        r_event(m)
        f_event(n)
        for item in work.get(n, ()):
            item()

    for a in range(HEADS):
        for d in range(1, RING):
            kv_send(a, d).wait_send()
            q_send(a, d).wait_send()
            pc = partner(d)
            o_send(a, pc).wait_send()
            remote(o_dst(pc, a), o_dst(pc, a), idx_ss.at[0], o_rs.at[a, pc], nxt).wait_recv()
        o_local(a).wait()
    for d in range(1, RING):
        id_send(d).wait_send()

    @when(has_next)
    def _():
        for slot in range(SLOTS - 1):
            @when(plane >= slot)
            def _():
                id_forward(slot).wait_send()
                for c in range(RING):
                    forward(0, slot, c).wait_send()
                for c in range(RING if slot == 0 else 1):
                    forward(1, slot, c).wait_send()

    for k in range(BACKS):
        @when(plane <= LAST_BACK)
        def _():
            back_own(k).wait_send()

        for i in range(3):
            @when(around(i + 1) <= LAST_BACK)
            def _():
                back_relay(i, k).wait_send()

        for slot in (4, 3):
            @when(jnp.logical_and(plane >= slot, plane != ZRING))
            def _():
                back_next(slot, k).wait_send()

        for e in range(2):
            @when(jnp.logical_or(plane == 0, jnp.logical_or(plane == 1, plane == 1 + e)))
            def _():
                ext_down(e, k, ext.at[e, k]).wait_send()


def local(queries, keys_values, segment_ids):
    dma = pltpu.SemaphoreType.DMA
    return pl.pallas_call(
        kernel,
        out_shape=jax.ShapeDtypeStruct(queries.shape, queries.dtype),
        in_specs=[
            pl.BlockSpec(memory_space=pl.ANY),
            pl.BlockSpec(memory_space=pl.ANY),
            pl.BlockSpec(memory_space=pltpu.VMEM),
        ],
        out_specs=pl.BlockSpec(memory_space=pl.ANY),
        scratch_shapes=[
            pltpu.VMEM((HEADS, RING, ROWS, WIDE), jnp.bfloat16),
            pltpu.VMEM((HEADS, SLOTS, 2, PLANE, DH), jnp.bfloat16),
            pltpu.VMEM((3, BACKS, 2, ROWS, DH), jnp.bfloat16),
            pltpu.VMEM((SLOTS, RING, 1, ROWS), jnp.int32),
            pltpu.VMEM((RING, ROWS, ROWS), jnp.int32),
            pltpu.VMEM((HEADS, RING, GROUP * ROWS, DH), jnp.float32),
            pltpu.VMEM((HEADS, RING, GROUP * ROWS, DH), jnp.float32),
            pltpu.VMEM((HEADS, RING, GROUP * ROWS, DH), jnp.float32),
            pltpu.VMEM((HEADS, RING, ROWS, WIDE), jnp.bfloat16),
            dma((3 * HEADS,)),
            dma((HEADS, RING - 1)),
            dma((HEADS, SLOTS, RING)),
            dma((HEADS, SLOTS - 1, RING)),
            dma((HEADS, RING - 1)),
            dma((HEADS, RING)),
            dma((RING - 1,)),
            dma((RING,)),
            dma((SLOTS - 1,)),
            dma((SLOTS,)),
            dma((HEADS, RING)),
            dma((HEADS, RING)),
            dma((BACKS,)),
            dma((3, BACKS)),
            dma((3, BACKS)),
            dma((2, BACKS)),
            pltpu.VMEM((2, BACKS, 2, ROWS, DH), jnp.bfloat16),
            dma((2, BACKS)),
            dma((2, BACKS)),
        ],
        compiler_params=pltpu.CompilerParams(collective_id=0, has_side_effects=True),
        name="window_attention",
    )(queries, keys_values, segment_ids.reshape(1, ROWS))


def solution(mesh):
    return jax.shard_map(
        local,
        mesh=mesh,
        in_specs=(P(("rep", "seq"), None), P(None, ("rep", "seq"), None), P(("rep", "seq"))),
        out_specs=P(("rep", "seq"), None),
        check_vma=False,
    )
```

```python
import math

import jax
import jax.numpy as jnp
from jax import lax
from jax.experimental import pallas as pl
from jax.experimental.pallas import tpu as pltpu
from jax.sharding import PartitionSpec as P

HQ = 32
HK = 8
DH = 128
WINDOW = 2048

RING = 4
ROWS = 128
PLANE = RING * ROWS
SLOTS = WINDOW // PLANE + 1
GROUP = HQ // HK
HEADS = HK // RING
WIDE = GROUP * DH
NEG_BIG = -1e30
SCALE = DH**-0.5 * math.log2(math.e)
MESH = pl.DeviceIdType.MESH
ZRING = 8
PLANES = 16
BACK = HEADS - 1
BACKS = RING - 1
LAST_BACK = PLANES - 3
F_EVENTS = 24
R_LAG = 10
R_EARLY = 8
R_EVENTS = 4 * BACKS


def kernel(
    q_hbm, kv_hbm, id_in, o_hbm,
    qbuf, kvb, rel, idb, qidc, m_sc, l_sc, acc_sc, obuf,
    loc_sem, kvx_ss, kv_rs, z_ss, qx_ss, q_rs, idx_ss, id0_rs, idz_ss, idz_rs, o_ss, o_rs,
    back_ss, rel_ss, rel_rs, rz_ss, side_ss,
):
    me = lax.axis_index("seq")
    x = lax.rem(me, RING)
    plane = me // RING
    half = plane // ZRING
    z = lax.rem(plane, ZRING)
    has_next = plane < PLANES - 1
    ring_base = plane * RING
    nxt = lax.rem(me + RING, PLANES * RING)
    prv = lax.rem(me + (PLANES - 1) * RING, PLANES * RING)

    def around(k):
        return half * ZRING + lax.rem(z + k, ZRING)

    third = around(3)
    relay = around(ZRING - 3) * RING + x

    def partner(d):
        return lax.rem(x + d, RING)

    def remote(src, dst, ss, rs, seq):
        return pltpu.make_async_remote_copy(
            src_ref=src, dst_ref=dst, send_sem=ss, recv_sem=rs,
            device_id={"seq": seq}, device_id_type=MESH,
        )

    def kv_src(px, a):
        return kv_hbm.at[:, :, pl.ds(pl.multiple_of((px * HEADS + a) * DH, DH), DH)]

    def q_src(px, a):
        return q_hbm.at[:, pl.ds(pl.multiple_of((px * HEADS + a) * WIDE, WIDE), WIDE)]

    def o_dst(px, a):
        return o_hbm.at[:, pl.ds(pl.multiple_of((px * HEADS + a) * WIDE, WIDE), WIDE)]

    def rows(c):
        return pl.ds(c * ROWS if isinstance(c, int) else pl.multiple_of(c * ROWS, ROWS), ROWS)

    def chunk(a, slot, c):
        return kvb.at[a, slot, :, rows(c), :]

    def signal(sem, seq):
        pl.semaphore_signal(sem, inc=1, device_id={"seq": seq}, device_id_type=MESH)

    def when(cond):
        return pl.when(cond)

    kv_local = [pltpu.make_async_copy(kv_src(x, a), chunk(a, 0, x), loc_sem.at[a]) for a in range(HEADS)]
    q_local = [pltpu.make_async_copy(q_src(x, a), qbuf.at[a, x], loc_sem.at[HEADS + a]) for a in range(HEADS)]
    for cp in kv_local + q_local:
        cp.start()
    idb[0, x] = id_in[...]

    barrier = pltpu.get_barrier_semaphore()
    for d in range(1, RING):
        signal(barrier, ring_base + partner(d))
    signal(barrier, third * RING + x)

    @when(plane > 0)
    def _():
        signal(barrier, prv)

    def last_relay(source):
        h = source // ZRING
        return (h * ZRING + lax.rem(source + ZRING - 3, ZRING)) * RING + x

    @when(plane >= SLOTS - 1)
    def _():
        signal(barrier, last_relay(plane - (SLOTS - 1)))

    @when(plane == PLANES - 1)
    def _():
        signal(barrier, last_relay(PLANES - 4))
        signal(barrier, last_relay(PLANES - 3))

    @when(jnp.logical_and(jnp.logical_and(plane >= 2, plane != ZRING - 1), has_next))
    def _():
        signal(barrier, nxt)

    @when(plane == ZRING - 1)
    def _():
        signal(barrier, RING + x)
        signal(barrier, 2 * RING + x)

    helper = jnp.logical_or(plane == 1, plane == 2)
    targets = (has_next, third <= LAST_BACK, jnp.logical_and(plane >= 3, plane != ZRING), helper)
    count = jnp.int32(RING)
    for target in targets:
        count = count + jnp.where(target, 1, 0)
    pl.semaphore_wait(barrier, count)

    def id_send(d):
        return remote(id_in, idb.at[0, x], idx_ss.at[d - 1], id0_rs.at[x], ring_base + partner(d))

    def kv_send(a, d):
        px = partner(d)
        return remote(kv_src(px, a), chunk(a, 0, x), kvx_ss.at[a, d - 1], kv_rs.at[a, 0, x], ring_base + px)

    def q_send(a, d):
        px = partner(d)
        return remote(q_src(px, a), qbuf.at[a, x], qx_ss.at[a, d - 1], q_rs.at[a, x], ring_base + px)

    def own_forward(a):
        return remote(kv_src(x, a), chunk(a, 1, x), z_ss.at[a, 0, x], kv_rs.at[a, 1, x], nxt)

    def forward(a, slot, c):
        return remote(chunk(a, slot, c), chunk(a, slot + 1, c), z_ss.at[a, slot, c], kv_rs.at[a, slot + 1, c], nxt)

    def id_forward(slot):
        return remote(idb.at[slot], idb.at[slot + 1], idz_ss.at[slot], idz_rs.at[slot + 1], nxt)

    def wait_chunk(a, slot, c):
        remote(chunk(a, slot, c), chunk(a, slot, c), kvx_ss.at[0, 0], kv_rs.at[a, slot, c], nxt).wait_recv()

    def back_own(k):
        return remote(chunk(BACK, 0, k + 1), rel.at[k], back_ss.at[k], rel_rs.at[k], relay)

    def back_relay(k):
        over = jnp.maximum(third - (PLANES - SLOTS), 0)
        slot = SLOTS - 1 - over
        first = jnp.minimum(third + SLOTS - 1, PLANES - 1) * RING + x
        return remote(rel.at[k], chunk(BACK, slot, k + 1), rel_ss.at[k], kv_rs.at[BACK, slot, k + 1], first)

    def back_side(k):
        slot = 4 - plane
        return remote(
            rel.at[k], chunk(BACK, slot, k + 1), side_ss.at[k], kv_rs.at[BACK, slot, k + 1], (ZRING - 1) * RING + x
        )

    def back_next(slot, k):
        return remote(
            chunk(BACK, slot, k + 1), chunk(BACK, slot - 1, k + 1),
            rz_ss.at[slot - 2, k], kv_rs.at[BACK, slot - 1, k + 1], prv,
        )

    def o_send(a, qb):
        return remote(obuf.at[a, qb], o_dst(x, a), o_ss.at[a, qb], o_rs.at[a, x], ring_base + qb)

    def o_local(a):
        return pltpu.make_async_copy(obuf.at[a, x], o_dst(x, a), loc_sem.at[2 * HEADS + a])

    @when(has_next)
    def _():
        own_forward(0).start()

    @when(jnp.logical_and(has_next, jnp.logical_or(plane != ZRING - 1, x == 0)))
    def _():
        own_forward(1).start()

    for d in range(1, RING):
        id_send(d).start()
    for a in range(HEADS):
        for d in (1, 3, 2):
            kv_send(a, d).start()
    for a in range(HEADS):
        for d in (1, 3, 2):
            q_send(a, d).start()

    kv_local[0].wait()
    for j in (1, 3, 2):
        wait_chunk(0, 0, partner(j))

        @when(has_next)
        def _():
            forward(0, 0, partner(j)).start()

    for d in range(1, RING):
        pc = partner(d)
        remote(idb.at[0, pc], idb.at[0, pc], idx_ss.at[0], id0_rs.at[pc], nxt).wait_recv()

    @when(has_next)
    def _():
        id_forward(0).start()

    def back_start(c):
        @when(jnp.logical_and(plane <= LAST_BACK, c > 0))
        def _():
            back_own(c - 1).start()

    kv_local[1].wait()
    back_start(x)
    for j in (1, 3, 2):
        wait_chunk(1, 0, partner(j))
        back_start(partner(j))

    @when(jnp.logical_and(has_next, x != 0))
    def _():
        forward(1, 0, 0).start()

    rest_late = jnp.logical_and(has_next, jnp.logical_and(plane != ZRING - 1, plane != ZRING))
    for cc in range(1, RING):
        @when(jnp.logical_and(plane == ZRING, cc != x))
        def _():
            forward(1, 0, cc).start()

    def f_event(n):
        if n < 5:
            a, slot, c = (0, 1, x) if n == 0 else (1, 1, x) if n == 1 else (0, 1, partner((1, 3, 2)[n - 2]))
        elif n < 21:
            k = n - 6
            a, slot, c = 0, 2 + k // 5, partner((0, 1, 3, 2, 0)[k % 5])
            if n % 5 == 0:
                a, slot, c = 1, n // 5, 0
        else:
            a, slot, c = 1, 1, n - 20
        if n in (0, 6, 11, 16):
            @when(plane >= slot)
            def _():
                remote(idb.at[slot], idb.at[slot], idx_ss.at[0], idz_rs.at[slot], nxt).wait_recv()

                if slot < SLOTS - 1:
                    @when(has_next)
                    def _():
                        id_forward(slot).start()

        there = plane >= slot
        if n == 1:
            there = jnp.logical_and(there, jnp.logical_or(plane != ZRING, x == 0))
        if n == 5:
            there = jnp.logical_and(there, c != x)
        if n > 20:
            there = jnp.logical_and(there, jnp.logical_or(plane == ZRING, c != x))

        @when(there)
        def _():
            wait_chunk(a, slot, c)

        if slot < SLOTS - 1 and n != 1 and n <= 20:
            @when(jnp.logical_and(plane >= slot, has_next))
            def _():
                forward(a, slot, c).start()

        if n == 15:
            for cc in range(1, RING):
                @when(jnp.logical_and(rest_late, cc != x))
                def _():
                    forward(1, 0, cc).start()

    def r_event(m):
        step, k = m // BACKS, m % BACKS
        if step == 0:
            @when(third <= LAST_BACK)
            def _():
                remote(rel.at[k], rel.at[k], idx_ss.at[0], rel_rs.at[k], nxt).wait_recv()
                back_relay(k).start()

            @when(helper)
            def _():
                back_side(k).start()
        else:
            slot = SLOTS - step
            on = plane != ZRING
            if slot == 2:
                on = plane == ZRING + 1

            @when(plane >= slot)
            def _():
                wait_chunk(BACK, slot, k + 1)

                @when(on)
                def _():
                    back_next(slot, k).start()

    row = lax.broadcasted_iota(jnp.int32, (ROWS, ROWS), 0)
    col = lax.broadcasted_iota(jnp.int32, (ROWS, ROWS), 1)

    def start_block(a, qb):
        @when(qb != x)
        def _():
            remote(qbuf.at[a, qb], qbuf.at[a, qb], idx_ss.at[0], q_rs.at[a, qb], nxt).wait_recv()

        @when(qb == x)
        def _():
            q_local[a].wait()

        m_sc[a, qb] = jnp.full((GROUP * ROWS, DH), NEG_BIG, jnp.float32)
        l_sc[a, qb] = jnp.zeros((GROUP * ROWS, DH), jnp.float32)
        acc_sc[a, qb] = jnp.zeros((GROUP * ROWS, DH), jnp.float32)
        if a == 0:
            qidc[qb] = jnp.transpose(jnp.broadcast_to(idb[0, qb], (ROWS, ROWS)))

    def blocks(a, slot, spans):
        ids = [idb[slot, c] for c in range(RING)]
        state, scores = [], []
        for qb, c0, c1 in spans:
            query_ids = qidc[qb]
            bias = []
            for c in range(c0, c1):
                keep = query_ids == ids[c]
                if slot == 0 and isinstance(qb, int) and c == qb:
                    keep = keep & (row >= col)
                if slot == SLOTS - 1 and isinstance(qb, int) and c == qb:
                    keep = keep & (col > row)
                bias.append(jnp.where(keep, 0.0, NEG_BIG))
            bias = jnp.concatenate(bias, axis=1)
            q_all = qbuf[a, qb]
            q4 = jnp.concatenate([q_all[:, g * DH : (g + 1) * DH] for g in range(GROUP)], axis=0)
            keys = kvb[a, slot, 0, c0 * ROWS : c1 * ROWS, :]
            state.append((m_sc[a, qb], l_sc[a, qb], acc_sc[a, qb]))
            s = lax.dot_general(q4, keys, (((1,), (1,)), ((), ())), preferred_element_type=jnp.float32)
            scores.append(s + jnp.concatenate([bias] * GROUP, axis=0))
        new = []
        for (qb, c0, c1), (m_prev, l_prev, acc_prev), s in zip(spans, state, scores):
            values = kvb[a, slot, 1, c0 * ROWS : c1 * ROWS, :]
            m_new = jnp.maximum(m_prev, jnp.max(s, axis=1, keepdims=True))
            alpha = jnp.exp2((m_prev - m_new) * SCALE)
            p = jnp.exp2((s - jnp.concatenate([m_new] * (c1 - c0), axis=1)) * SCALE)
            part = p[:, :ROWS]
            for c in range(1, c1 - c0):
                part = part + p[:, c * ROWS : (c + 1) * ROWS]
            acc = acc_prev * alpha + jnp.dot(p.astype(jnp.bfloat16), values, preferred_element_type=jnp.float32)
            new.append((m_new, l_prev * alpha + part, acc))
        for (qb, _, _), (m_new, l_new, acc) in zip(spans, new):
            m_sc[a, qb] = m_new
            l_sc[a, qb] = l_new
            acc_sc[a, qb] = acc

    def inner(a, slot, lo, hi):
        @when(plane >= slot)
        def _():
            blocks(a, slot, [(qb, 0, RING) for qb in range(lo, hi)])

    def diagonal(a, lo, hi):
        for qb in range(lo, hi):
            start_block(a, qb)
        blocks(a, 0, [(qb, 0, qb + 1) for qb in range(lo, hi)])

    def edge(a, lo, hi):
        @when(plane >= SLOTS - 1)
        def _():
            blocks(a, SLOTS - 1, [(qb, qb, RING) for qb in range(lo, hi)])

    def finish(a, lo, hi):
        for qb in range(lo, hi):
            out = acc_sc[a, qb] / jnp.sum(l_sc[a, qb], axis=1, keepdims=True)
            for g in range(GROUP):
                obuf[a, qb, :, g * DH : (g + 1) * DH] = out[g * ROWS : (g + 1) * ROWS].astype(jnp.bfloat16)

            @when(qb != x)
            def _():
                o_send(a, qb).start()

            @when(qb == x)
            def _():
                o_local(a).start()

    def near(lo, hi):
        @when(plane >= 1)
        def _():
            def one(k, carry):
                qb = 2 * k
                blocks(BACK, 1, [(qb, lo, hi), (qb + 1, lo, hi)])
                return carry

            lax.fori_loop(0, RING // 2, one, 0)

    work = {
        6: [lambda: diagonal(0, 0, 4)],
        7: [lambda: inner(0, 1, 0, 2)],
        8: [lambda: inner(0, 1, 2, 4)],
        10: [lambda: inner(0, 2, 0, 2)],
        11: [lambda: inner(0, 2, 2, 4)],
        12: [lambda: diagonal(1, 0, 4)],
        14: [lambda: inner(0, 3, 0, 2)],
        15: [lambda: inner(0, 3, 2, 4)],
        18: [lambda: inner(1, 3, 0, 4)],
        19: [lambda: edge(0, 0, 4), lambda: finish(0, 0, 4)],
        20: [lambda: edge(1, 0, 4)],
        21: [lambda: inner(1, 2, 0, 4)],
        22: [lambda: near(0, 3)],
        23: [lambda: near(3, 4), lambda: finish(1, 0, 4)],
    }
    early = plane == ZRING
    for n in range(F_EVENTS):
        for mine, first, rest in ((early, 4, 10), (jnp.logical_not(early), 10, 10)):
            ms = [m for m in range(R_EVENTS) if m + (first if m < BACKS else rest) == n]
            if ms:
                @when(mine)
                def _():
                    for m in ms:
                        r_event(m)
        f_event(n)
        for item in work.get(n, ()):
            item()

    for a in range(HEADS):
        for d in range(1, RING):
            kv_send(a, d).wait_send()
            q_send(a, d).wait_send()
            pc = partner(d)
            o_send(a, pc).wait_send()
            remote(o_dst(pc, a), o_dst(pc, a), idx_ss.at[0], o_rs.at[a, pc], nxt).wait_recv()
        o_local(a).wait()
    for d in range(1, RING):
        id_send(d).wait_send()

    @when(has_next)
    def _():
        for slot in range(SLOTS - 1):
            @when(plane >= slot)
            def _():
                id_forward(slot).wait_send()
                for c in range(RING):
                    forward(0, slot, c).wait_send()
                forward(1, slot, 0).wait_send()
                if slot == 0:
                    @when(plane != ZRING - 1)
                    def _():
                        for c in range(1, RING):
                            forward(1, slot, c).wait_send()

    for k in range(BACKS):
        @when(plane <= LAST_BACK)
        def _():
            back_own(k).wait_send()

        @when(third <= LAST_BACK)
        def _():
            back_relay(k).wait_send()

        @when(helper)
        def _():
            back_side(k).wait_send()

        for slot in (4, 3, 2):
            on = plane != ZRING
            if slot == 2:
                on = plane == ZRING + 1

            @when(jnp.logical_and(plane >= slot, on))
            def _():
                back_next(slot, k).wait_send()


def local(queries, keys_values, segment_ids):
    dma = pltpu.SemaphoreType.DMA
    return pl.pallas_call(
        kernel,
        out_shape=jax.ShapeDtypeStruct(queries.shape, queries.dtype),
        in_specs=[
            pl.BlockSpec(memory_space=pltpu.HBM),
            pl.BlockSpec(memory_space=pltpu.HBM),
            pl.BlockSpec(memory_space=pltpu.VMEM),
        ],
        out_specs=pl.BlockSpec(memory_space=pl.ANY),
        scratch_shapes=[
            pltpu.VMEM((HEADS, RING, ROWS, WIDE), jnp.bfloat16),
            pltpu.VMEM((HEADS, SLOTS, 2, PLANE, DH), jnp.bfloat16),
            pltpu.VMEM((BACKS, 2, ROWS, DH), jnp.bfloat16),
            pltpu.VMEM((SLOTS, RING, 1, ROWS), jnp.int32),
            pltpu.VMEM((RING, ROWS, ROWS), jnp.int32),
            pltpu.VMEM((HEADS, RING, GROUP * ROWS, DH), jnp.float32),
            pltpu.VMEM((HEADS, RING, GROUP * ROWS, DH), jnp.float32),
            pltpu.VMEM((HEADS, RING, GROUP * ROWS, DH), jnp.float32),
            pltpu.VMEM((HEADS, RING, ROWS, WIDE), jnp.bfloat16),
            dma((3 * HEADS,)),
            dma((HEADS, RING - 1)),
            dma((HEADS, SLOTS, RING)),
            dma((HEADS, SLOTS - 1, RING)),
            dma((HEADS, RING - 1)),
            dma((HEADS, RING)),
            dma((RING - 1,)),
            dma((RING,)),
            dma((SLOTS - 1,)),
            dma((SLOTS,)),
            dma((HEADS, RING)),
            dma((HEADS, RING)),
            dma((BACKS,)),
            dma((BACKS,)),
            dma((BACKS,)),
            dma((3, BACKS)),
            dma((BACKS,)),
        ],
        compiler_params=pltpu.CompilerParams(collective_id=0, has_side_effects=True, vmem_limit_bytes=32 * 1024 * 1024),
        name="window_attention",
    )(
        pltpu.with_memory_space_constraint(queries, pltpu.HBM),
        pltpu.with_memory_space_constraint(keys_values, pltpu.HBM),
        segment_ids.reshape(1, ROWS),
    )


def solution(mesh):
    return jax.shard_map(
        local,
        mesh=mesh,
        in_specs=(P(("rep", "seq"), None), P(None, ("rep", "seq"), None), P(("rep", "seq"))),
        out_specs=P(("rep", "seq"), None),
        check_vma=False,
    )
```

```python
import math

import jax
import jax.numpy as jnp
from jax import lax
from jax.experimental import pallas as pl
from jax.experimental.pallas import tpu as pltpu
from jax.sharding import PartitionSpec as P

HQ = 32
HK = 8
DH = 128
WINDOW = 2048

RING = 4
ROWS = 128
PLANE = RING * ROWS
SLOTS = WINDOW // PLANE + 1
GROUP = HQ // HK
HEADS = HK // RING
WIDE = GROUP * DH
NEG_BIG = -1e30
SCALE = DH**-0.5 * math.log2(math.e)
MESH = pl.DeviceIdType.MESH
ZRING = 8
PLANES = 16
BACK = HEADS - 1
BACKS = RING - 1
LAST_BACK = PLANES - 3
F_EVENTS = 24
R_LAG = 10
R_EARLY = 8
R_EVENTS = 4 * BACKS


def kernel(
    q_hbm, kv_hbm, id_in, o_hbm,
    qbuf, kvb, rel, idb, qidc, m_sc, l_sc, acc_sc, obuf,
    loc_sem, kvx_ss, kv_rs, z_ss, qx_ss, q_rs, idx_ss, id0_rs, idz_ss, idz_rs, o_ss, o_rs,
    back_ss, rel_ss, rel_rs, rz_ss, side_ss,
):
    me = lax.axis_index("seq")
    x = lax.rem(me, RING)
    plane = me // RING
    half = plane // ZRING
    z = lax.rem(plane, ZRING)
    has_next = plane < PLANES - 1
    ring_base = plane * RING
    nxt = lax.rem(me + RING, PLANES * RING)
    prv = lax.rem(me + (PLANES - 1) * RING, PLANES * RING)

    def around(k):
        return half * ZRING + lax.rem(z + k, ZRING)

    third = around(3)
    relay = around(ZRING - 3) * RING + x

    def partner(d):
        return lax.rem(x + d, RING)

    def remote(src, dst, ss, rs, seq):
        return pltpu.make_async_remote_copy(
            src_ref=src, dst_ref=dst, send_sem=ss, recv_sem=rs,
            device_id={"seq": seq}, device_id_type=MESH,
        )

    def kv_src(px, a):
        return kv_hbm.at[:, :, pl.ds(pl.multiple_of((px * HEADS + a) * DH, DH), DH)]

    def q_src(px, a):
        return q_hbm.at[:, pl.ds(pl.multiple_of((px * HEADS + a) * WIDE, WIDE), WIDE)]

    def o_dst(px, a):
        return o_hbm.at[:, pl.ds(pl.multiple_of((px * HEADS + a) * WIDE, WIDE), WIDE)]

    def rows(c):
        return pl.ds(c * ROWS if isinstance(c, int) else pl.multiple_of(c * ROWS, ROWS), ROWS)

    def chunk(a, slot, c):
        return kvb.at[a, slot, :, rows(c), :]

    def signal(sem, seq):
        pl.semaphore_signal(sem, inc=1, device_id={"seq": seq}, device_id_type=MESH)

    def when(cond):
        return pl.when(cond)

    kv_local = [pltpu.make_async_copy(kv_src(x, a), chunk(a, 0, x), loc_sem.at[a]) for a in range(HEADS)]
    q_local = [pltpu.make_async_copy(q_src(x, a), qbuf.at[a, x], loc_sem.at[HEADS + a]) for a in range(HEADS)]
    for cp in kv_local + q_local:
        cp.start()
    idb[0, x] = id_in[...]

    barrier = pltpu.get_barrier_semaphore()
    for d in range(1, RING):
        signal(barrier, ring_base + partner(d))
    signal(barrier, third * RING + x)

    @when(plane > 0)
    def _():
        signal(barrier, prv)

    def last_relay(source):
        h = source // ZRING
        return (h * ZRING + lax.rem(source + ZRING - 3, ZRING)) * RING + x

    @when(plane >= SLOTS - 1)
    def _():
        signal(barrier, last_relay(plane - (SLOTS - 1)))

    @when(plane == PLANES - 1)
    def _():
        signal(barrier, last_relay(PLANES - 4))
        signal(barrier, last_relay(PLANES - 3))

    @when(jnp.logical_and(jnp.logical_and(plane >= 2, plane != ZRING - 1), has_next))
    def _():
        signal(barrier, nxt)

    @when(plane == ZRING - 1)
    def _():
        signal(barrier, RING + x)
        signal(barrier, 2 * RING + x)

    helper = jnp.logical_or(plane == 1, plane == 2)
    targets = (has_next, third <= LAST_BACK, jnp.logical_and(plane >= 3, plane != ZRING), helper)
    count = jnp.int32(RING)
    for target in targets:
        count = count + jnp.where(target, 1, 0)
    pl.semaphore_wait(barrier, count)

    def id_send(d):
        return remote(id_in, idb.at[0, x], idx_ss.at[d - 1], id0_rs.at[x], ring_base + partner(d))

    def kv_send(a, d):
        px = partner(d)
        return remote(kv_src(px, a), chunk(a, 0, x), kvx_ss.at[a, d - 1], kv_rs.at[a, 0, x], ring_base + px)

    def q_send(a, d):
        px = partner(d)
        return remote(q_src(px, a), qbuf.at[a, x], qx_ss.at[a, d - 1], q_rs.at[a, x], ring_base + px)

    def own_forward(a):
        return remote(kv_src(x, a), chunk(a, 1, x), z_ss.at[a, 0, x], kv_rs.at[a, 1, x], nxt)

    def forward(a, slot, c):
        return remote(chunk(a, slot, c), chunk(a, slot + 1, c), z_ss.at[a, slot, c], kv_rs.at[a, slot + 1, c], nxt)

    def id_forward(slot):
        return remote(idb.at[slot], idb.at[slot + 1], idz_ss.at[slot], idz_rs.at[slot + 1], nxt)

    def wait_chunk(a, slot, c):
        remote(chunk(a, slot, c), chunk(a, slot, c), kvx_ss.at[0, 0], kv_rs.at[a, slot, c], nxt).wait_recv()

    def back_own(k):
        return remote(chunk(BACK, 0, k + 1), rel.at[k], back_ss.at[k], rel_rs.at[k], relay)

    def back_relay(k):
        over = jnp.maximum(third - (PLANES - SLOTS), 0)
        slot = SLOTS - 1 - over
        first = jnp.minimum(third + SLOTS - 1, PLANES - 1) * RING + x
        return remote(rel.at[k], chunk(BACK, slot, k + 1), rel_ss.at[k], kv_rs.at[BACK, slot, k + 1], first)

    def back_side(k):
        slot = 4 - plane
        return remote(
            rel.at[k], chunk(BACK, slot, k + 1), side_ss.at[k], kv_rs.at[BACK, slot, k + 1], (ZRING - 1) * RING + x
        )

    def back_next(slot, k):
        return remote(
            chunk(BACK, slot, k + 1), chunk(BACK, slot - 1, k + 1),
            rz_ss.at[slot - 2, k], kv_rs.at[BACK, slot - 1, k + 1], prv,
        )

    def o_send(a, qb):
        return remote(obuf.at[a, qb], o_dst(x, a), o_ss.at[a, qb], o_rs.at[a, x], ring_base + qb)

    def o_local(a):
        return pltpu.make_async_copy(obuf.at[a, x], o_dst(x, a), loc_sem.at[2 * HEADS + a])

    @when(has_next)
    def _():
        own_forward(0).start()

    @when(jnp.logical_and(has_next, jnp.logical_or(plane != ZRING - 1, x == 0)))
    def _():
        own_forward(1).start()

    for d in range(1, RING):
        id_send(d).start()
    for a in range(HEADS):
        for d in (1, 3, 2):
            kv_send(a, d).start()
    for a in range(HEADS):
        for d in (1, 3, 2):
            q_send(a, d).start()

    kv_local[0].wait()
    for j in (1, 3, 2):
        wait_chunk(0, 0, partner(j))

        @when(has_next)
        def _():
            forward(0, 0, partner(j)).start()

    for d in range(1, RING):
        pc = partner(d)
        remote(idb.at[0, pc], idb.at[0, pc], idx_ss.at[0], id0_rs.at[pc], nxt).wait_recv()

    @when(has_next)
    def _():
        id_forward(0).start()

    def back_start(c):
        @when(jnp.logical_and(plane <= LAST_BACK, c > 0))
        def _():
            back_own(c - 1).start()

    kv_local[1].wait()
    back_start(x)
    for j in (1, 3, 2):
        wait_chunk(1, 0, partner(j))
        back_start(partner(j))

    @when(jnp.logical_and(has_next, x != 0))
    def _():
        forward(1, 0, 0).start()

    rest_late = jnp.logical_and(has_next, jnp.logical_and(plane != ZRING - 1, plane != ZRING))
    for cc in range(1, RING):
        @when(jnp.logical_and(plane == ZRING, cc != x))
        def _():
            forward(1, 0, cc).start()

    def f_event(n):
        if n < 5:
            a, slot, c = (0, 1, x) if n == 0 else (1, 1, x) if n == 1 else (0, 1, partner((1, 3, 2)[n - 2]))
        elif n < 21:
            k = n - 6
            a, slot, c = 0, 2 + k // 5, partner((0, 1, 3, 2, 0)[k % 5])
            if n % 5 == 0:
                a, slot, c = 1, n // 5, 0
        else:
            a, slot, c = 1, 1, n - 20
        if n in (0, 6, 11, 16):
            @when(plane >= slot)
            def _():
                remote(idb.at[slot], idb.at[slot], idx_ss.at[0], idz_rs.at[slot], nxt).wait_recv()

                if slot < SLOTS - 1:
                    @when(has_next)
                    def _():
                        id_forward(slot).start()

        there = plane >= slot
        if n == 1:
            there = jnp.logical_and(there, jnp.logical_or(plane != ZRING, x == 0))
        if n == 5:
            there = jnp.logical_and(there, c != x)
        if n > 20:
            there = jnp.logical_and(there, jnp.logical_or(plane == ZRING, c != x))

        @when(there)
        def _():
            wait_chunk(a, slot, c)

        if slot < SLOTS - 1 and n != 1 and n <= 20:
            @when(jnp.logical_and(plane >= slot, has_next))
            def _():
                forward(a, slot, c).start()

        if n == 15:
            for cc in range(1, RING):
                @when(jnp.logical_and(rest_late, cc != x))
                def _():
                    forward(1, 0, cc).start()

    def r_event(m):
        step, k = m // BACKS, m % BACKS
        if step == 0:
            @when(third <= LAST_BACK)
            def _():
                remote(rel.at[k], rel.at[k], idx_ss.at[0], rel_rs.at[k], nxt).wait_recv()
                back_relay(k).start()

            @when(helper)
            def _():
                back_side(k).start()
        else:
            slot = SLOTS - step
            on = plane != ZRING
            if slot == 2:
                on = plane == ZRING + 1

            @when(plane >= slot)
            def _():
                wait_chunk(BACK, slot, k + 1)

                @when(on)
                def _():
                    back_next(slot, k).start()

    row = lax.broadcasted_iota(jnp.int32, (ROWS, ROWS), 0)
    col = lax.broadcasted_iota(jnp.int32, (ROWS, ROWS), 1)

    def start_block(a, qb):
        @when(qb != x)
        def _():
            remote(qbuf.at[a, qb], qbuf.at[a, qb], idx_ss.at[0], q_rs.at[a, qb], nxt).wait_recv()

        @when(qb == x)
        def _():
            q_local[a].wait()

        m_sc[a, qb] = jnp.full((GROUP * ROWS, DH), NEG_BIG, jnp.float32)
        l_sc[a, qb] = jnp.zeros((GROUP * ROWS, DH), jnp.float32)
        acc_sc[a, qb] = jnp.zeros((GROUP * ROWS, DH), jnp.float32)
        if a == 0:
            qidc[qb] = jnp.transpose(jnp.broadcast_to(idb[0, qb], (ROWS, ROWS)))

    def blocks(a, slot, spans):
        ids = [idb[slot, c] for c in range(RING)]
        state, scores = [], []
        for qb, c0, c1 in spans:
            query_ids = qidc[qb]
            bias = []
            for c in range(c0, c1):
                keep = query_ids == ids[c]
                if slot == 0 and isinstance(qb, int) and c == qb:
                    keep = keep & (row >= col)
                if slot == SLOTS - 1 and isinstance(qb, int) and c == qb:
                    keep = keep & (col > row)
                bias.append(jnp.where(keep, 0.0, NEG_BIG))
            bias = jnp.concatenate(bias, axis=1)
            q_all = qbuf[a, qb]
            q4 = jnp.concatenate([q_all[:, g * DH : (g + 1) * DH] for g in range(GROUP)], axis=0)
            keys = kvb[a, slot, 0, c0 * ROWS : c1 * ROWS, :]
            state.append((m_sc[a, qb], l_sc[a, qb], acc_sc[a, qb]))
            s = lax.dot_general(q4, keys, (((1,), (1,)), ((), ())), preferred_element_type=jnp.float32)
            scores.append(s + jnp.concatenate([bias] * GROUP, axis=0))
        new = []
        for (qb, c0, c1), (m_prev, l_prev, acc_prev), s in zip(spans, state, scores):
            values = kvb[a, slot, 1, c0 * ROWS : c1 * ROWS, :]
            m_new = jnp.maximum(m_prev, jnp.max(s, axis=1, keepdims=True))
            alpha = jnp.exp2((m_prev - m_new) * SCALE)
            p = jnp.exp2((s - jnp.concatenate([m_new] * (c1 - c0), axis=1)) * SCALE)
            part = p[:, :ROWS]
            for c in range(1, c1 - c0):
                part = part + p[:, c * ROWS : (c + 1) * ROWS]
            acc = acc_prev * alpha + jnp.dot(p.astype(jnp.bfloat16), values, preferred_element_type=jnp.float32)
            new.append((m_new, l_prev * alpha + part, acc))
        for (qb, _, _), (m_new, l_new, acc) in zip(spans, new):
            m_sc[a, qb] = m_new
            l_sc[a, qb] = l_new
            acc_sc[a, qb] = acc

    def inner(a, slot, lo, hi):
        @when(plane >= slot)
        def _():
            blocks(a, slot, [(qb, 0, RING) for qb in range(lo, hi)])

    def diagonal(a, lo, hi):
        for qb in range(lo, hi):
            start_block(a, qb)
        blocks(a, 0, [(qb, 0, qb + 1) for qb in range(lo, hi)])

    def edge(a, lo, hi):
        @when(plane >= SLOTS - 1)
        def _():
            blocks(a, SLOTS - 1, [(qb, qb, RING) for qb in range(lo, hi)])

    def finish(a, lo, hi):
        for qb in range(lo, hi):
            out = acc_sc[a, qb] / jnp.sum(l_sc[a, qb], axis=1, keepdims=True)
            for g in range(GROUP):
                obuf[a, qb, :, g * DH : (g + 1) * DH] = out[g * ROWS : (g + 1) * ROWS].astype(jnp.bfloat16)

            @when(qb != x)
            def _():
                o_send(a, qb).start()

            @when(qb == x)
            def _():
                o_local(a).start()

    def near(lo, hi, first=0, last=RING):
        @when(plane >= 1)
        def _():
            blocks(BACK, 1, [(qb, lo, hi) for qb in range(first, last)])

    work = {
        6: [lambda: diagonal(0, 0, 4)],
        7: [lambda: inner(0, 1, 0, 2)],
        8: [lambda: inner(0, 1, 2, 4)],
        10: [lambda: inner(0, 2, 0, 2)],
        11: [lambda: inner(0, 2, 2, 4)],
        12: [lambda: diagonal(1, 0, 4)],
        14: [lambda: inner(0, 3, 0, 2)],
        15: [lambda: inner(0, 3, 2, 4)],
        18: [lambda: inner(1, 3, 0, 4)],
        19: [lambda: edge(0, 0, 4), lambda: finish(0, 0, 4)],
        20: [lambda: edge(1, 0, 4)],
        21: [lambda: inner(1, 2, 0, 2)],
        22: [lambda: near(0, 3, 0, 2)],
        23: [
            lambda: near(3, 4, 0, 2), lambda: finish(1, 0, 2),
            lambda: inner(1, 2, 2, 4), lambda: near(0, 4, 2, 4), lambda: finish(1, 2, 4),
        ],
    }
    early = plane == ZRING
    for n in range(F_EVENTS):
        for mine, first, rest in ((early, 4, 10), (jnp.logical_not(early), 10, 10)):
            ms = [m for m in range(R_EVENTS) if m + (first if m < BACKS else rest) == n]
            if ms:
                @when(mine)
                def _():
                    for m in ms:
                        r_event(m)
        f_event(n)
        for item in work.get(n, ()):
            item()

    for a in range(HEADS):
        for d in range(1, RING):
            kv_send(a, d).wait_send()
            q_send(a, d).wait_send()
            pc = partner(d)
            o_send(a, pc).wait_send()
            remote(o_dst(pc, a), o_dst(pc, a), idx_ss.at[0], o_rs.at[a, pc], nxt).wait_recv()
        o_local(a).wait()
    for d in range(1, RING):
        id_send(d).wait_send()

    @when(has_next)
    def _():
        for slot in range(SLOTS - 1):
            @when(plane >= slot)
            def _():
                id_forward(slot).wait_send()
                for c in range(RING):
                    forward(0, slot, c).wait_send()
                forward(1, slot, 0).wait_send()
                if slot == 0:
                    @when(plane != ZRING - 1)
                    def _():
                        for c in range(1, RING):
                            forward(1, slot, c).wait_send()

    for k in range(BACKS):
        @when(plane <= LAST_BACK)
        def _():
            back_own(k).wait_send()

        @when(third <= LAST_BACK)
        def _():
            back_relay(k).wait_send()

        @when(helper)
        def _():
            back_side(k).wait_send()

        for slot in (4, 3, 2):
            on = plane != ZRING
            if slot == 2:
                on = plane == ZRING + 1

            @when(jnp.logical_and(plane >= slot, on))
            def _():
                back_next(slot, k).wait_send()


def local(queries, keys_values, segment_ids):
    dma = pltpu.SemaphoreType.DMA
    return pl.pallas_call(
        kernel,
        out_shape=jax.ShapeDtypeStruct(queries.shape, queries.dtype),
        in_specs=[
            pl.BlockSpec(memory_space=pltpu.HBM),
            pl.BlockSpec(memory_space=pltpu.HBM),
            pl.BlockSpec(memory_space=pltpu.VMEM),
        ],
        out_specs=pl.BlockSpec(memory_space=pl.ANY),
        scratch_shapes=[
            pltpu.VMEM((HEADS, RING, ROWS, WIDE), jnp.bfloat16),
            pltpu.VMEM((HEADS, SLOTS, 2, PLANE, DH), jnp.bfloat16),
            pltpu.VMEM((BACKS, 2, ROWS, DH), jnp.bfloat16),
            pltpu.VMEM((SLOTS, RING, 1, ROWS), jnp.int32),
            pltpu.VMEM((RING, ROWS, ROWS), jnp.int32),
            pltpu.VMEM((HEADS, RING, GROUP * ROWS, DH), jnp.float32),
            pltpu.VMEM((HEADS, RING, GROUP * ROWS, DH), jnp.float32),
            pltpu.VMEM((HEADS, RING, GROUP * ROWS, DH), jnp.float32),
            pltpu.VMEM((HEADS, RING, ROWS, WIDE), jnp.bfloat16),
            dma((3 * HEADS,)),
            dma((HEADS, RING - 1)),
            dma((HEADS, SLOTS, RING)),
            dma((HEADS, SLOTS - 1, RING)),
            dma((HEADS, RING - 1)),
            dma((HEADS, RING)),
            dma((RING - 1,)),
            dma((RING,)),
            dma((SLOTS - 1,)),
            dma((SLOTS,)),
            dma((HEADS, RING)),
            dma((HEADS, RING)),
            dma((BACKS,)),
            dma((BACKS,)),
            dma((BACKS,)),
            dma((3, BACKS)),
            dma((BACKS,)),
        ],
        compiler_params=pltpu.CompilerParams(collective_id=0, has_side_effects=True, vmem_limit_bytes=32 * 1024 * 1024),
        name="window_attention",
    )(
        pltpu.with_memory_space_constraint(queries, pltpu.HBM),
        pltpu.with_memory_space_constraint(keys_values, pltpu.HBM),
        segment_ids.reshape(1, ROWS),
    )


def solution(mesh):
    return jax.shard_map(
        local,
        mesh=mesh,
        in_specs=(P(("rep", "seq"), None), P(None, ("rep", "seq"), None), P(("rep", "seq"))),
        out_specs=P(("rep", "seq"), None),
        check_vma=False,
    )
```

```python
import math

import jax
import jax.numpy as jnp
from jax import lax
from jax.experimental import pallas as pl
from jax.experimental.pallas import tpu as pltpu
from jax.sharding import PartitionSpec as P

HQ = 32
HK = 8
DH = 128
WINDOW = 2048

RING = 4
ROWS = 128
PLANE = RING * ROWS
SLOTS = WINDOW // PLANE + 1
GROUP = HQ // HK
HEADS = HK // RING
WIDE = GROUP * DH
NEG_BIG = -1e30
SCALE = DH**-0.5 * math.log2(math.e)
MESH = pl.DeviceIdType.MESH
ZRING = 8
PLANES = 16
BACK = HEADS - 1
BACKS = RING - 1
LAST_BACK = PLANES - 3
F_EVENTS = 24
R_LAG = 10
R_EARLY = 8
R_EVENTS = 4 * BACKS


def kernel(
    q_hbm, kv_hbm, id_in, o_hbm,
    qbuf, kvb, rel, idb, qidc, m_sc, l_sc, acc_sc, obuf,
    loc_sem, kvx_ss, kv_rs, z_ss, qx_ss, q_rs, idx_ss, id0_rs, idz_ss, idz_rs, o_ss, o_rs,
    back_ss, rel_ss, rel_rs, rz_ss, side_ss,
):
    me = lax.axis_index("seq")
    x = lax.rem(me, RING)
    plane = me // RING
    half = plane // ZRING
    z = lax.rem(plane, ZRING)
    has_next = plane < PLANES - 1
    ring_base = plane * RING
    nxt = lax.rem(me + RING, PLANES * RING)
    prv = lax.rem(me + (PLANES - 1) * RING, PLANES * RING)

    def around(k):
        return half * ZRING + lax.rem(z + k, ZRING)

    third = around(3)
    relay = around(ZRING - 3) * RING + x

    def partner(d):
        return lax.rem(x + d, RING)

    def remote(src, dst, ss, rs, seq):
        return pltpu.make_async_remote_copy(
            src_ref=src, dst_ref=dst, send_sem=ss, recv_sem=rs,
            device_id={"seq": seq}, device_id_type=MESH,
        )

    def kv_src(px, a):
        return kv_hbm.at[:, :, pl.ds(pl.multiple_of((px * HEADS + a) * DH, DH), DH)]

    def q_src(px, a):
        return q_hbm.at[:, pl.ds(pl.multiple_of((px * HEADS + a) * WIDE, WIDE), WIDE)]

    def o_dst(px, a):
        return o_hbm.at[:, pl.ds(pl.multiple_of((px * HEADS + a) * WIDE, WIDE), WIDE)]

    def rows(c):
        return pl.ds(c * ROWS if isinstance(c, int) else pl.multiple_of(c * ROWS, ROWS), ROWS)

    def chunk(a, slot, c):
        return kvb.at[a, slot, :, rows(c), :]

    def signal(sem, seq):
        pl.semaphore_signal(sem, inc=1, device_id={"seq": seq}, device_id_type=MESH)

    def when(cond):
        return pl.when(cond)

    barrier = pltpu.get_barrier_semaphore()

    @when(plane > 0)
    def _():
        signal(barrier, prv)

    for d in range(1, RING):
        signal(barrier, ring_base + partner(d))
    signal(barrier, third * RING + x)

    def last_relay(source):
        h = source // ZRING
        return (h * ZRING + lax.rem(source + ZRING - 3, ZRING)) * RING + x

    @when(plane >= SLOTS - 1)
    def _():
        signal(barrier, last_relay(plane - (SLOTS - 1)))

    @when(plane == PLANES - 1)
    def _():
        signal(barrier, last_relay(PLANES - 4))
        signal(barrier, last_relay(PLANES - 3))

    @when(jnp.logical_and(jnp.logical_and(plane >= 2, plane != ZRING - 1), has_next))
    def _():
        signal(barrier, nxt)

    @when(plane == ZRING - 1)
    def _():
        signal(barrier, RING + x)
        signal(barrier, 2 * RING + x)

    kv_local = [pltpu.make_async_copy(kv_src(x, a), chunk(a, 0, x), loc_sem.at[a]) for a in range(HEADS)]
    q_local = [pltpu.make_async_copy(q_src(x, a), qbuf.at[a, x], loc_sem.at[HEADS + a]) for a in range(HEADS)]
    for cp in kv_local + q_local:
        cp.start()
    idb[0, x] = id_in[...]

    helper = jnp.logical_or(plane == 1, plane == 2)
    targets = (has_next, third <= LAST_BACK, jnp.logical_and(plane >= 3, plane != ZRING), helper)
    count = jnp.int32(RING)
    for target in targets:
        count = count + jnp.where(target, 1, 0)
    pl.semaphore_wait(barrier, count)

    def id_send(d):
        return remote(id_in, idb.at[0, x], idx_ss.at[d - 1], id0_rs.at[x], ring_base + partner(d))

    def kv_send(a, d):
        px = partner(d)
        return remote(kv_src(px, a), chunk(a, 0, x), kvx_ss.at[a, d - 1], kv_rs.at[a, 0, x], ring_base + px)

    def q_send(a, d):
        px = partner(d)
        return remote(q_src(px, a), qbuf.at[a, x], qx_ss.at[a, d - 1], q_rs.at[a, x], ring_base + px)

    def own_forward(a):
        return remote(kv_src(x, a), chunk(a, 1, x), z_ss.at[a, 0, x], kv_rs.at[a, 1, x], nxt)

    def forward(a, slot, c):
        return remote(chunk(a, slot, c), chunk(a, slot + 1, c), z_ss.at[a, slot, c], kv_rs.at[a, slot + 1, c], nxt)

    def id_forward(slot):
        return remote(idb.at[slot], idb.at[slot + 1], idz_ss.at[slot], idz_rs.at[slot + 1], nxt)

    def wait_chunk(a, slot, c):
        remote(chunk(a, slot, c), chunk(a, slot, c), kvx_ss.at[0, 0], kv_rs.at[a, slot, c], nxt).wait_recv()

    def back_own(k):
        return remote(chunk(BACK, 0, k + 1), rel.at[k], back_ss.at[k], rel_rs.at[k], relay)

    def back_relay(k):
        over = jnp.maximum(third - (PLANES - SLOTS), 0)
        slot = SLOTS - 1 - over
        first = jnp.minimum(third + SLOTS - 1, PLANES - 1) * RING + x
        return remote(rel.at[k], chunk(BACK, slot, k + 1), rel_ss.at[k], kv_rs.at[BACK, slot, k + 1], first)

    def back_side(k):
        slot = 4 - plane
        return remote(
            rel.at[k], chunk(BACK, slot, k + 1), side_ss.at[k], kv_rs.at[BACK, slot, k + 1], (ZRING - 1) * RING + x
        )

    def back_next(slot, k):
        return remote(
            chunk(BACK, slot, k + 1), chunk(BACK, slot - 1, k + 1),
            rz_ss.at[slot - 2, k], kv_rs.at[BACK, slot - 1, k + 1], prv,
        )

    def o_send(a, qb):
        return remote(obuf.at[a, qb], o_dst(x, a), o_ss.at[a, qb], o_rs.at[a, x], ring_base + qb)

    def o_local(a):
        return pltpu.make_async_copy(obuf.at[a, x], o_dst(x, a), loc_sem.at[2 * HEADS + a])

    @when(has_next)
    def _():
        own_forward(0).start()

    @when(jnp.logical_and(has_next, jnp.logical_or(plane != ZRING - 1, x == 0)))
    def _():
        own_forward(1).start()

    for d in range(1, RING):
        id_send(d).start()
    for a in range(HEADS):
        for d in (1, 3, 2):
            kv_send(a, d).start()
    for a in range(HEADS):
        for d in (1, 3, 2):
            q_send(a, d).start()

    kv_local[0].wait()
    for j in (1, 3, 2):
        wait_chunk(0, 0, partner(j))

        @when(has_next)
        def _():
            forward(0, 0, partner(j)).start()

    for d in range(1, RING):
        pc = partner(d)
        remote(idb.at[0, pc], idb.at[0, pc], idx_ss.at[0], id0_rs.at[pc], nxt).wait_recv()

    @when(has_next)
    def _():
        id_forward(0).start()

    def back_start(c):
        @when(jnp.logical_and(plane <= LAST_BACK, c > 0))
        def _():
            back_own(c - 1).start()

    kv_local[1].wait()
    back_start(x)
    for j in (1, 3, 2):
        wait_chunk(1, 0, partner(j))
        back_start(partner(j))

    @when(jnp.logical_and(has_next, x != 0))
    def _():
        forward(1, 0, 0).start()

    rest_late = jnp.logical_and(has_next, jnp.logical_and(plane != ZRING - 1, plane != ZRING))
    for cc in range(1, RING):
        @when(jnp.logical_and(plane == ZRING, cc != x))
        def _():
            forward(1, 0, cc).start()

    def f_event(n):
        if n < 5:
            a, slot, c = (0, 1, x) if n == 0 else (1, 1, x) if n == 1 else (0, 1, partner((1, 3, 2)[n - 2]))
        elif n < 21:
            k = n - 6
            a, slot, c = 0, 2 + k // 5, partner((0, 1, 3, 2, 0)[k % 5])
            if n % 5 == 0:
                a, slot, c = 1, n // 5, 0
        else:
            a, slot, c = 1, 1, n - 20
        if n in (0, 6, 11, 16):
            @when(plane >= slot)
            def _():
                remote(idb.at[slot], idb.at[slot], idx_ss.at[0], idz_rs.at[slot], nxt).wait_recv()

                if slot < SLOTS - 1:
                    @when(has_next)
                    def _():
                        id_forward(slot).start()

        there = plane >= slot
        if n == 1:
            there = jnp.logical_and(there, jnp.logical_or(plane != ZRING, x == 0))
        if n == 5:
            there = jnp.logical_and(there, c != x)
        if n > 20:
            there = jnp.logical_and(there, jnp.logical_or(plane == ZRING, c != x))

        @when(there)
        def _():
            wait_chunk(a, slot, c)

        if slot < SLOTS - 1 and n != 1 and n <= 20:
            @when(jnp.logical_and(plane >= slot, has_next))
            def _():
                forward(a, slot, c).start()

        if n == 15:
            for cc in range(1, RING):
                @when(jnp.logical_and(rest_late, cc != x))
                def _():
                    forward(1, 0, cc).start()

    def r_event(m):
        step, k = m // BACKS, m % BACKS
        if step == 0:
            @when(third <= LAST_BACK)
            def _():
                remote(rel.at[k], rel.at[k], idx_ss.at[0], rel_rs.at[k], nxt).wait_recv()
                back_relay(k).start()

            @when(helper)
            def _():
                back_side(k).start()
        else:
            slot = SLOTS - step
            on = plane != ZRING
            if slot == 2:
                on = plane == ZRING + 1

            @when(plane >= slot)
            def _():
                wait_chunk(BACK, slot, k + 1)

                @when(on)
                def _():
                    back_next(slot, k).start()

    row = lax.broadcasted_iota(jnp.int32, (ROWS, ROWS), 0)
    col = lax.broadcasted_iota(jnp.int32, (ROWS, ROWS), 1)

    def start_block(a, qb):
        @when(qb != x)
        def _():
            remote(qbuf.at[a, qb], qbuf.at[a, qb], idx_ss.at[0], q_rs.at[a, qb], nxt).wait_recv()

        @when(qb == x)
        def _():
            q_local[a].wait()

        m_sc[a, qb] = jnp.full((GROUP * ROWS, DH), NEG_BIG, jnp.float32)
        l_sc[a, qb] = jnp.zeros((GROUP * ROWS, DH), jnp.float32)
        acc_sc[a, qb] = jnp.zeros((GROUP * ROWS, DH), jnp.float32)
        if a == 0:
            qidc[qb] = jnp.transpose(jnp.broadcast_to(idb[0, qb], (ROWS, ROWS)))

    def blocks(a, slot, spans):
        ids = [idb[slot, c] for c in range(RING)]
        state, scores = [], []
        for qb, c0, c1 in spans:
            query_ids = qidc[qb]
            bias = []
            for c in range(c0, c1):
                keep = query_ids == ids[c]
                if slot == 0 and isinstance(qb, int) and c == qb:
                    keep = keep & (row >= col)
                if slot == SLOTS - 1 and isinstance(qb, int) and c == qb:
                    keep = keep & (col > row)
                bias.append(jnp.where(keep, 0.0, NEG_BIG))
            bias = jnp.concatenate(bias, axis=1)
            q_all = qbuf[a, qb]
            q4 = jnp.concatenate([q_all[:, g * DH : (g + 1) * DH] for g in range(GROUP)], axis=0)
            keys = kvb[a, slot, 0, c0 * ROWS : c1 * ROWS, :]
            state.append((m_sc[a, qb], l_sc[a, qb], acc_sc[a, qb]))
            s = lax.dot_general(q4, keys, (((1,), (1,)), ((), ())), preferred_element_type=jnp.float32)
            scores.append(s + jnp.concatenate([bias] * GROUP, axis=0))
        new = []
        for (qb, c0, c1), (m_prev, l_prev, acc_prev), s in zip(spans, state, scores):
            values = kvb[a, slot, 1, c0 * ROWS : c1 * ROWS, :]
            m_new = jnp.maximum(m_prev, jnp.max(s, axis=1, keepdims=True))
            alpha = jnp.exp2((m_prev - m_new) * SCALE)
            p = jnp.exp2((s - jnp.concatenate([m_new] * (c1 - c0), axis=1)) * SCALE)
            part = p[:, :ROWS]
            for c in range(1, c1 - c0):
                part = part + p[:, c * ROWS : (c + 1) * ROWS]
            acc = acc_prev * alpha + jnp.dot(p.astype(jnp.bfloat16), values, preferred_element_type=jnp.float32)
            new.append((m_new, l_prev * alpha + part, acc))
        for (qb, _, _), (m_new, l_new, acc) in zip(spans, new):
            m_sc[a, qb] = m_new
            l_sc[a, qb] = l_new
            acc_sc[a, qb] = acc

    def inner(a, slot, lo, hi):
        @when(plane >= slot)
        def _():
            blocks(a, slot, [(qb, 0, RING) for qb in range(lo, hi)])

    def diagonal(a, lo, hi):
        for qb in range(lo, hi):
            start_block(a, qb)
        blocks(a, 0, [(qb, 0, qb + 1) for qb in range(lo, hi)])

    def edge(a, lo, hi):
        @when(plane >= SLOTS - 1)
        def _():
            blocks(a, SLOTS - 1, [(qb, qb, RING) for qb in range(lo, hi)])

    def finish(a, lo, hi):
        for qb in range(lo, hi):
            out = acc_sc[a, qb] / jnp.sum(l_sc[a, qb], axis=1, keepdims=True)
            for g in range(GROUP):
                obuf[a, qb, :, g * DH : (g + 1) * DH] = out[g * ROWS : (g + 1) * ROWS].astype(jnp.bfloat16)

            @when(qb != x)
            def _():
                o_send(a, qb).start()

            @when(qb == x)
            def _():
                o_local(a).start()

    def near(lo, hi, first=0, last=RING):
        @when(plane >= 1)
        def _():
            blocks(BACK, 1, [(qb, lo, hi) for qb in range(first, last)])

    work = {
        6: [lambda: diagonal(0, 0, 4)],
        7: [lambda: inner(0, 1, 0, 2)],
        8: [lambda: inner(0, 1, 2, 4)],
        10: [lambda: inner(0, 2, 0, 2)],
        11: [lambda: inner(0, 2, 2, 4)],
        12: [lambda: diagonal(1, 0, 4)],
        14: [lambda: inner(0, 3, 0, 2)],
        15: [lambda: inner(0, 3, 2, 4)],
        18: [lambda: inner(1, 3, 0, 4)],
        19: [lambda: edge(0, 0, 4), lambda: finish(0, 0, 4)],
        20: [lambda: edge(1, 0, 4)],
        21: [lambda: inner(1, 2, 0, 2)],
        22: [lambda: near(0, 3, 0, 2)],
        23: [
            lambda: near(3, 4, 0, 2), lambda: finish(1, 0, 2),
            lambda: inner(1, 2, 2, 4), lambda: near(0, 4, 2, 4), lambda: finish(1, 2, 4),
        ],
    }
    early = plane == ZRING
    for n in range(F_EVENTS):
        for mine, ticks in (
            (early, [4, 5, 6] + [18] * 6 + [21] * 3),
            (plane == ZRING + 1, [m + 10 for m in range(R_EVENTS)]),
            ((plane != ZRING) & (plane != ZRING + 1), [m + 10 for m in range(9)] + [21] * 3),
        ):
            ms = [m for m in range(R_EVENTS) if ticks[m] == n]
            if ms:
                @when(mine)
                def _():
                    for m in ms:
                        r_event(m)
        f_event(n)
        for item in work.get(n, ()):
            item()

    for a in range(HEADS):
        for d in range(1, RING):
            kv_send(a, d).wait_send()
            q_send(a, d).wait_send()
            pc = partner(d)
            o_send(a, pc).wait_send()
            remote(o_dst(pc, a), o_dst(pc, a), idx_ss.at[0], o_rs.at[a, pc], nxt).wait_recv()
        o_local(a).wait()
    for d in range(1, RING):
        id_send(d).wait_send()

    @when(has_next)
    def _():
        for slot in range(SLOTS - 1):
            @when(plane >= slot)
            def _():
                id_forward(slot).wait_send()
                for c in range(RING):
                    forward(0, slot, c).wait_send()
                forward(1, slot, 0).wait_send()
                if slot == 0:
                    @when(plane != ZRING - 1)
                    def _():
                        for c in range(1, RING):
                            forward(1, slot, c).wait_send()

    for k in range(BACKS):
        @when(plane <= LAST_BACK)
        def _():
            back_own(k).wait_send()

        @when(third <= LAST_BACK)
        def _():
            back_relay(k).wait_send()

        @when(helper)
        def _():
            back_side(k).wait_send()

        for slot in (4, 3, 2):
            on = plane != ZRING
            if slot == 2:
                on = plane == ZRING + 1

            @when(jnp.logical_and(plane >= slot, on))
            def _():
                back_next(slot, k).wait_send()


def local(queries, keys_values, segment_ids):
    dma = pltpu.SemaphoreType.DMA
    return pl.pallas_call(
        kernel,
        out_shape=jax.ShapeDtypeStruct(queries.shape, queries.dtype),
        in_specs=[
            pl.BlockSpec(memory_space=pltpu.HBM),
            pl.BlockSpec(memory_space=pltpu.HBM),
            pl.BlockSpec(memory_space=pltpu.VMEM),
        ],
        out_specs=pl.BlockSpec(memory_space=pl.ANY),
        scratch_shapes=[
            pltpu.VMEM((HEADS, RING, ROWS, WIDE), jnp.bfloat16),
            pltpu.VMEM((HEADS, SLOTS, 2, PLANE, DH), jnp.bfloat16),
            pltpu.VMEM((BACKS, 2, ROWS, DH), jnp.bfloat16),
            pltpu.VMEM((SLOTS, RING, 1, ROWS), jnp.int32),
            pltpu.VMEM((RING, ROWS, ROWS), jnp.int32),
            pltpu.VMEM((HEADS, RING, GROUP * ROWS, DH), jnp.float32),
            pltpu.VMEM((HEADS, RING, GROUP * ROWS, DH), jnp.float32),
            pltpu.VMEM((HEADS, RING, GROUP * ROWS, DH), jnp.float32),
            pltpu.VMEM((HEADS, RING, ROWS, WIDE), jnp.bfloat16),
            dma((3 * HEADS,)),
            dma((HEADS, RING - 1)),
            dma((HEADS, SLOTS, RING)),
            dma((HEADS, SLOTS - 1, RING)),
            dma((HEADS, RING - 1)),
            dma((HEADS, RING)),
            dma((RING - 1,)),
            dma((RING,)),
            dma((SLOTS - 1,)),
            dma((SLOTS,)),
            dma((HEADS, RING)),
            dma((HEADS, RING)),
            dma((BACKS,)),
            dma((BACKS,)),
            dma((BACKS,)),
            dma((3, BACKS)),
            dma((BACKS,)),
        ],
        compiler_params=pltpu.CompilerParams(collective_id=0, has_side_effects=True, vmem_limit_bytes=32 * 1024 * 1024),
        name="window_attention",
    )(
        pltpu.with_memory_space_constraint(queries, pltpu.HBM),
        pltpu.with_memory_space_constraint(keys_values, pltpu.HBM),
        segment_ids.reshape(1, ROWS),
    )


def solution(mesh):
    return jax.shard_map(
        local,
        mesh=mesh,
        in_specs=(P(("rep", "seq"), None), P(None, ("rep", "seq"), None), P(("rep", "seq"))),
        out_specs=P(("rep", "seq"), None),
        check_vma=False,
    )
```
